128 devices in a mesh: dp: 1, tp: 2 (over core), sp: 64 (over z, y, x).
Axes of the slice: x: 4, y: 4, z: 4, core: 2. Of those that a mesh axis runs over, the one named last changes fastest.
Arguments:
- hidden: bfloat16 [32, 6144], P('dp')
- norm_w: bfloat16 [6144], replicated
- w_q: bfloat16 [6144, 6144], P(None, 'tp')
- b_q: bfloat16 [6144], P('tp')
- w_k: bfloat16 [6144, 256], P(None, 'tp')
- b_k: bfloat16 [256], P('tp')
- w_v: bfloat16 [6144, 256], P(None, 'tp')
- b_v: bfloat16 [256], P('tp')
- w_o: bfloat16 [6144, 6144], P('tp')
- k_cache: bfloat16 [32, 32768, 2, 128], P('dp', 'sp', 'tp')
- v_cache: bfloat16 [32, 32768, 2, 128], P('dp', 'sp', 'tp')
- positions: int32 [32], P('dp')
- seq_lens: int32 [32], P('dp')
Outputs:
- output 1: bfloat16 [32, 6144], P('dp')
- output 2: bfloat16 [32, 2, 128], P('dp', 'tp')
- output 3: bfloat16 [32, 2, 128], P('dp', 'tp')
All inputs are finite; a program needn't handle non-finite values.
Results may differ from the reference program's by a relative error of at most 0.00881808.
Values sent between devices are 32-bit elements.
A program may use at most 1 GiB of HBM per device.

```python
import jax
import jax.numpy as jnp
from jax import lax

BATCH = 32
SEQ_LEN = 32768
D_MODEL = 6144
N_HEADS = 48
KV_GROUPS = 2
HEAD_DIM = 128
ROT_DIM = HEAD_DIM // 2
PER_GROUP = N_HEADS // KV_GROUPS
Q_COLS = N_HEADS * HEAD_DIM
KV_COLS = KV_GROUPS * HEAD_DIM
RMS_EPS = 1.5625e-7
ROPE_BASE = 10000.0


def normal_draw(key, shape, std):
    return std * jax.random.normal(key, shape, jnp.float32)


def setup_inputs(seed: int = 0, part: int = 0) -> dict:
    shared_keys = jax.random.split(jax.random.key(seed), 8)
    part_keys = jax.random.split(jax.random.fold_in(jax.random.key(seed + 1), part), 5)
    val_scale = (SEQ_LEN ** 0.5) / 4.0
    cache_shape = (BATCH, SEQ_LEN, KV_GROUPS, HEAD_DIM)
    seq_lens = jax.random.randint(part_keys[3], (BATCH,), SEQ_LEN // 8, SEQ_LEN + 1, dtype=jnp.int32)
    seq_lens = seq_lens.at[0].set(SEQ_LEN).at[1].set(SEQ_LEN // 8)
    positions = seq_lens + jax.random.randint(part_keys[4], (BATCH,), 0, SEQ_LEN + 1, dtype=jnp.int32)
    return {
        'hidden': normal_draw(part_keys[0], (BATCH, D_MODEL), 1.0).astype(jnp.bfloat16),
        'norm_w': (1.0 + normal_draw(shared_keys[0], (D_MODEL,), 0.3)).astype(jnp.bfloat16),
        'w_q': normal_draw(shared_keys[1], (D_MODEL, Q_COLS), D_MODEL ** -0.5).astype(jnp.bfloat16),
        'b_q': normal_draw(shared_keys[2], (Q_COLS,), 0.5).astype(jnp.bfloat16),
        'w_k': normal_draw(shared_keys[3], (D_MODEL, KV_COLS), D_MODEL ** -0.5).astype(jnp.bfloat16),
        'b_k': normal_draw(shared_keys[4], (KV_COLS,), 0.5).astype(jnp.bfloat16),
        'w_v': normal_draw(shared_keys[5], (D_MODEL, KV_COLS), D_MODEL ** -0.5).astype(jnp.bfloat16),
        'b_v': normal_draw(shared_keys[6], (KV_COLS,), 0.5).astype(jnp.bfloat16),
        'w_o': normal_draw(shared_keys[7], (Q_COLS, D_MODEL), Q_COLS ** -0.5).astype(jnp.bfloat16),
        'k_cache': normal_draw(part_keys[1], cache_shape, 1.4).astype(jnp.bfloat16),
        'v_cache': normal_draw(part_keys[2], cache_shape, val_scale).astype(jnp.bfloat16),
        'positions': positions,
        'seq_lens': seq_lens,
    }


def apply_rotary(heads_in, positions):
    half_rot = ROT_DIM // 2
    inv_freq = ROPE_BASE ** (-2.0 * jnp.arange(half_rot, dtype=jnp.float32) / ROT_DIM)
    angles = positions.astype(jnp.float32)[:, None, None] * inv_freq
    cos_t = jnp.cos(angles)
    sin_t = jnp.sin(angles)
    rot_pairs = heads_in[..., :ROT_DIM].astype(jnp.float32).reshape(heads_in.shape[:-1] + (half_rot, 2))
    even_part = rot_pairs[..., 0]
    odd_part = rot_pairs[..., 1]
    rotated = jnp.stack([even_part * cos_t - odd_part * sin_t, even_part * sin_t + odd_part * cos_t], axis=-1)
    rotated = rotated.reshape(heads_in.shape[:-1] + (ROT_DIM,)).astype(jnp.bfloat16)
    return jnp.concatenate([rotated, heads_in[..., ROT_DIM:]], axis=-1)


def project(normed, weight, bias_vec):
    return (jnp.dot(normed, weight, preferred_element_type=jnp.float32) + bias_vec.astype(jnp.float32)).astype(jnp.bfloat16)


def reference(hidden, norm_w, w_q, b_q, w_k, b_k, w_v, b_v, w_o, k_cache, v_cache, positions, seq_lens):
    x_f32 = hidden.astype(jnp.float32)
    mean_sq = jnp.mean(x_f32 * x_f32, axis=-1, keepdims=True)
    normed = (x_f32 * lax.rsqrt(mean_sq + RMS_EPS) * norm_w.astype(jnp.float32)).astype(jnp.bfloat16)
    q_rot = apply_rotary(project(normed, w_q, b_q).reshape(BATCH, N_HEADS, HEAD_DIM), positions)
    k_rot = apply_rotary(project(normed, w_k, b_k).reshape(BATCH, KV_GROUPS, HEAD_DIM), positions)
    v_new = project(normed, w_v, b_v).reshape(BATCH, KV_GROUPS, HEAD_DIM)
    attn_scale = HEAD_DIM ** -0.5
    cache_idx = jnp.arange(SEQ_LEN)

    def one_row(row_args):
        q_row, k_row, v_row, k_tok, v_tok, length = row_args
        q_grp = q_row.reshape(KV_GROUPS, PER_GROUP, HEAD_DIM).astype(jnp.float32)
        s_cache = jnp.einsum('gqd,sgd->gqs', q_grp, k_row.astype(jnp.float32)) * attn_scale
        s_cache = jnp.where((cache_idx < length)[None, None, :], s_cache, -jnp.inf)
        s_new = jnp.einsum('gqd,gd->gq', q_grp, k_tok.astype(jnp.float32)) * attn_scale
        m_top = jnp.maximum(jnp.max(s_cache, axis=-1), s_new)
        p_cache = jnp.exp(s_cache - m_top[..., None])
        p_new = jnp.exp(s_new - m_top)
        exp_sum = jnp.sum(p_cache, axis=-1) + p_new
        weighted = jnp.einsum('gqs,sgd->gqd', p_cache, v_row.astype(jnp.float32))
        weighted = weighted + p_new[..., None] * v_tok.astype(jnp.float32)[:, None, :]
        return (weighted / exp_sum[..., None]).reshape(Q_COLS).astype(jnp.bfloat16)

    attn_rows = lax.map(one_row, (q_rot, k_cache, v_cache, k_rot, v_new, seq_lens))
    y_out = (x_f32 + jnp.dot(attn_rows, w_o, preferred_element_type=jnp.float32)).astype(jnp.bfloat16)
    return y_out, k_rot, v_new
```

```python
import functools
import math

import jax
import jax.numpy as jnp
from jax import lax
from jax.experimental import pallas as pl
from jax.experimental.pallas import tpu as pltpu
from jax.sharding import PartitionSpec as P

RMS_EPS = 1.5625e-7
ROPE_BASE = 10000.0
NEG_BIG = -3.0e38
MESH = pl.DeviceIdType.MESH
F32 = jnp.float32
BF16 = jnp.bfloat16

N_ROWS = 32
S_DEV = 512
D = 128
SP = 64
PLANE = 16
HALF = 12
SLOT = 16
N_OUT = 6144
N_Z = 1536
AG = 24
UNROLL = 4


def rms_norm(x_rows, norm_w):
    x_f32 = x_rows.astype(jnp.float32)
    mean_sq = jnp.mean(x_f32 * x_f32, axis=-1, keepdims=True)
    return (x_f32 * lax.rsqrt(mean_sq + RMS_EPS) * norm_w.astype(jnp.float32)).astype(jnp.bfloat16)


def apply_rotary(heads_in, positions):
    rot_dim = heads_in.shape[-1] // 2
    half_rot = rot_dim // 2
    inv_freq = ROPE_BASE ** (-2.0 * jnp.arange(half_rot, dtype=jnp.float32) / rot_dim)
    angles = positions.astype(jnp.float32)[:, None, None] * inv_freq
    cos_t = jnp.cos(angles)
    sin_t = jnp.sin(angles)
    rot_pairs = heads_in[..., :rot_dim].astype(jnp.float32).reshape(heads_in.shape[:-1] + (half_rot, 2))
    even_part = rot_pairs[..., 0]
    odd_part = rot_pairs[..., 1]
    rotated = jnp.stack([even_part * cos_t - odd_part * sin_t, even_part * sin_t + odd_part * cos_t], axis=-1)
    rotated = rotated.reshape(heads_in.shape[:-1] + (rot_dim,)).astype(jnp.bfloat16)
    return jnp.concatenate([rotated, heads_in[..., rot_dim:]], axis=-1)


def project(normed, weight, bias_vec):
    return (jnp.dot(normed, weight, preferred_element_type=jnp.float32) + bias_vec.astype(jnp.float32)).astype(jnp.bfloat16)


def tail_kernel(q_ref, kn_ref, vn_ref, seq_ref, hid_ref, k_hbm, v_hbm, wo_hbm, y_ref,
                kbuf, vbuf, wobuf, o_send, o_recv, a_all, lhs, ypart, yrecv, ag,
                ksem, vsem, wsem, rs_send, rs_recv, z_send, z_recv, d_send, d_recv,
                ag_send, ag_recv, f_send, f_recv):
    c = lax.axis_index('tp')
    s = lax.axis_index('sp')
    z = lax.div(s, PLANE)
    p = lax.rem(s, PLANE)
    qk_scale = (D ** -0.5) * math.log2(math.e)

    def chip_of(i):
        return lax.rem(p + 1 + lax.div(i, 2), PLANE)

    def row_of(i):
        return chip_of(i) + PLANE * lax.rem(i, 2)

    barrier = pltpu.get_barrier_semaphore()

    def greet(d, carry):
        pl.semaphore_signal(barrier, inc=1, device_id={'sp': lax.rem(s + d, SP)}, device_id_type=MESH)
        return carry
    lax.fori_loop(1, SP, greet, 0)
    pl.semaphore_signal(barrier, inc=1, device_id={'tp': 1 - c}, device_id_type=MESH)

    def k_copy(i):
        return pltpu.make_async_copy(k_hbm.at[row_of(i)], kbuf.at[i], ksem.at[i])

    def v_copy(i):
        return pltpu.make_async_copy(v_hbm.at[row_of(i)], vbuf.at[i], vsem.at[i])

    def start_kv(i, carry):
        k_copy(i).start()
        v_copy(i).start()
        return carry
    lax.fori_loop(0, N_ROWS, start_kv, 0)
    wo_copies = [pltpu.make_async_copy(
        wo_hbm.at[pl.ds(768 * j, 768), pl.ds(pl.multiple_of(z * N_Z, N_Z), N_Z)],
        wobuf.at[pl.ds(768 * j, 768)], wsem.at[j]) for j in range(4)]
    for cp in wo_copies:
        cp.start()

    pl.semaphore_wait(barrier, SP)

    lane = lax.broadcasted_iota(jnp.int32, (SLOT, D), 1)
    sub = lax.broadcasted_iota(jnp.int32, (SLOT, D), 0)
    eye = lane == sub
    pos = s * S_DEV + lax.broadcasted_iota(jnp.int32, (2 * SLOT, S_DEV), 1)

    def rs_copy(i, hf):
        dest = (2 * lax.rem(i, 2) + hf) * PLANE + chip_of(i)
        slot = 2 * i + hf
        return dest, pltpu.make_async_remote_copy(
            src_ref=o_send.at[slot], dst_ref=o_recv.at[pl.ds(pl.multiple_of(s * SLOT, SLOT), SLOT)],
            send_sem=rs_send, recv_sem=rs_recv, device_id={'sp': dest}, device_id_type=MESH)

    def rows_step(g, carry):
        idx = [g * UNROLL + u for u in range(UNROLL)]
        rows = [row_of(i) for i in idx]
        scores = []
        for i, b in zip(idx, rows):
            k_copy(i).wait()
            sc = lax.dot_general(q_ref[b], kbuf[i], (((1,), (1,)), ((), ())), preferred_element_type=F32)
            scores.append(jnp.where(pos < seq_ref[b], sc, NEG_BIG))
        tops = [jnp.max(sc, axis=1, keepdims=True) for sc in scores]
        probs = [jnp.exp2((sc - m) * qk_scale) for sc, m in zip(scores, tops)]
        sums = [jnp.sum(pr, axis=1, keepdims=True) for pr in probs]
        for i, m, l, pr in zip(idx, tops, sums, probs):
            v_copy(i).wait()
            o = jnp.dot(pr.astype(BF16), vbuf[i], preferred_element_type=F32)
            m2 = m * qk_scale
            for hf in range(2):
                part = slice(hf * SLOT, (hf + 1) * SLOT)
                m_row = jnp.sum(jnp.where(eye, m2[part], 0.0), axis=0, keepdims=True)
                l_row = jnp.sum(jnp.where(eye, l[part], 0.0), axis=0, keepdims=True)
                o_send[2 * i + hf] = jnp.where(sub == HALF, m_row, jnp.where(sub == HALF + 1, l_row, o[part]))
        for i in idx:
            for hf in range(2):
                dest, cp = rs_copy(i, hf)

                @pl.when(dest != s)
                def _():
                    cp.start()

                @pl.when(dest == s)
                def _():
                    o_recv[pl.ds(pl.multiple_of(s * SLOT, SLOT), SLOT), :] = o_send[2 * i + hf]
        return carry
    lax.fori_loop(0, N_ROWS // UNROLL, rows_step, 0)

    my_row = p + PLANE * lax.div(z, 2)
    my_half = lax.rem(z, 2)
    q_mine = q_ref[my_row, pl.ds(pl.multiple_of(my_half * SLOT, SLOT), SLOT), :].astype(F32)
    k_mine = kn_ref[my_row]
    v_mine = vn_ref[my_row]
    s_new = jnp.sum(q_mine * k_mine, axis=1, keepdims=True) * qk_scale

    def all_in(ref, sem):
        pltpu.make_async_copy(ref, ref, sem).wait()

    all_in(o_recv.at[pl.ds(0, (SP - 1) * SLOT)], rs_recv)
    m_rows = o_recv[pl.ds(HALF, SP, stride=SLOT), :]
    l_rows = o_recv[pl.ds(HALF + 1, SP, stride=SLOT), :]
    stats = jnp.transpose(jnp.concatenate([m_rows, l_rows], axis=0))[:SLOT]
    m_cols, l_cols = stats[:, :SP], stats[:, SP:]
    m_top = jnp.maximum(jnp.max(m_cols, axis=1, keepdims=True), s_new)
    w_cols = jnp.exp2(m_cols - m_top)
    w_new = jnp.exp2(s_new - m_top)
    l_all = jnp.sum(w_cols * l_cols, axis=1, keepdims=True) + w_new
    acc = w_new * v_mine
    for j in range(SP):
        acc = acc + w_cols[:, j:j + 1] * o_recv[j * SLOT:(j + 1) * SLOT, :]
    a_all[z] = acc / l_all

    z_copies = []
    for dz in range(1, 4):
        z_copies.append(pltpu.make_async_remote_copy(
            src_ref=a_all.at[z], dst_ref=a_all.at[z], send_sem=z_send.at[dz - 1], recv_sem=z_recv.at[dz - 1],
            device_id={'sp': lax.rem(z + dz, 4) * PLANE + p}, device_id_type=MESH))
    for cp in z_copies:
        cp.start()
    lhs[...] = jnp.zeros_like(lhs)
    for cp in z_copies:
        cp.wait_recv()
    for zz in range(4):
        r, hf = zz // 2, zz % 2
        for j in range(HALF):
            lhs[r:r + 1, (hf * HALF + j) * D:(hf * HALF + j + 1) * D] = a_all[zz, j:j + 1, :]
    for cp in wo_copies:
        cp.wait()
    ypart[0] = jnp.dot(lhs[...].astype(BF16), wobuf[...], preferred_element_type=F32)

    d_copy = pltpu.make_async_remote_copy(
        src_ref=ypart.at[0], dst_ref=ypart.at[1], send_sem=d_send, recv_sem=d_recv,
        device_id={'tp': 1 - c}, device_id_type=MESH)
    d_copy.start()
    d_copy.wait_recv()
    both = ypart[0] + ypart[1]

    def ag_slot(i):
        return ag.at[pl.ds(pl.multiple_of(i * AG, 8), AG)]

    for r in range(2):
        for blk in range(12):
            yrecv[r * 12 + blk:r * 12 + blk + 1, :] = both[r:r + 1, blk * D:(blk + 1) * D]
    ag[pl.ds(pl.multiple_of(s * AG, 8), AG), :] = yrecv[...]
    par = lax.rem(s + c, 2)

    def ag_copy(i):
        dest = 2 * i + par
        return dest, pltpu.make_async_remote_copy(
            src_ref=ag_slot(s), dst_ref=ag_slot(s), send_sem=ag_send.at[i], recv_sem=ag_recv.at[lax.div(s, 2)],
            device_id={'sp': dest}, device_id_type=MESH)

    def ag_start(i, carry):
        dest, cp = ag_copy(i)

        @pl.when(dest != s)
        def _():
            cp.start()
        return carry
    lax.fori_loop(0, SP // 2, ag_start, 0)

    def forward(i):
        return pltpu.make_async_remote_copy(
            src_ref=ag_slot(2 * i + par), dst_ref=ag_slot(2 * i + par), send_sem=f_send.at[i], recv_sem=f_recv.at[i],
            device_id={'tp': 1 - c}, device_id_type=MESH)

    def relay(i, carry):
        src = 2 * i + par

        @pl.when(src != s)
        def _():
            pltpu.make_async_copy(ag_slot(src), ag_slot(src), ag_recv.at[i]).wait()
            forward(i).start()
        return carry
    lax.fori_loop(0, SP // 2, relay, 0)

    def relayed(i, carry):
        src = 2 * i + 1 - par

        @pl.when(src != s)
        def _():
            pltpu.make_async_copy(ag_slot(src), ag_slot(src), f_recv.at[i]).wait()
        return carry
    lax.fori_loop(0, SP // 2, relayed, 0)

    for zz in range(4):
        for blk in range(12):
            col = slice(zz * N_Z + blk * D, zz * N_Z + (blk + 1) * D)
            for r in range(2):
                rows = slice(PLANE * r, PLANE * (r + 1))
                y_blk = ag[pl.ds(zz * PLANE * AG + r * 12 + blk, PLANE, stride=AG), :]
                y_ref[rows, col] = (hid_ref[rows, col].astype(F32) + y_blk).astype(BF16)

    all_in(o_send.at[pl.ds(0, SP - 1)], rs_send)
    for cp in z_copies:
        cp.wait_send()
    d_copy.wait_send()

    def drain(i, carry):
        dest, cp = ag_copy(i)

        @pl.when(dest != s)
        def _():
            cp.wait_send()

        @pl.when(2 * i + par != s)
        def _():
            forward(i).wait_send()
        return carry
    lax.fori_loop(0, SP // 2, drain, 0)


def tail(q_pad, k_new, v_new, seq_lens, hidden, k_cache, v_cache, w_o):
    vmem = pl.BlockSpec(memory_space=pltpu.VMEM)
    hbm = pl.BlockSpec(memory_space=pl.ANY)
    dma = pltpu.SemaphoreType.DMA
    return pl.pallas_call(
        tail_kernel,
        out_shape=jax.ShapeDtypeStruct((N_ROWS, N_OUT), BF16),
        in_specs=[vmem, vmem, vmem, pl.BlockSpec(memory_space=pltpu.SMEM), vmem, hbm, hbm, hbm],
        out_specs=vmem,
        scratch_shapes=[
            pltpu.VMEM((N_ROWS, S_DEV, D), BF16),
            pltpu.VMEM((N_ROWS, S_DEV, D), BF16),
            pltpu.VMEM((3072, N_Z), BF16),
            pltpu.VMEM((2 * N_ROWS, SLOT, D), F32),
            pltpu.VMEM((SP * SLOT, D), F32),
            pltpu.VMEM((4, SLOT, D), F32),
            pltpu.VMEM((8, 3072), F32),
            pltpu.VMEM((2, 8, N_Z), F32),
            pltpu.VMEM((AG, D), F32),
            pltpu.VMEM((SP * AG, D), F32),
            dma((N_ROWS,)), dma((N_ROWS,)), dma((4,)),
            dma, dma, dma((3,)), dma((3,)), dma, dma,
            dma((SP // 2,)), dma((SP // 2,)), dma((SP // 2,)), dma((SP // 2,)),
        ],
        compiler_params=pltpu.CompilerParams(
            collective_id=0, has_side_effects=True, vmem_limit_bytes=48 * 1024 * 1024),
        name='tail',
    )(q_pad, k_new, v_new, seq_lens, hidden, k_cache, v_cache, w_o)


def solution(mesh):
    def device_step(hidden, norm_w, w_q, b_q, w_k, b_k, w_v, b_v, w_o, k_cache, v_cache, positions, seq_lens):
        n_rows = hidden.shape[0]
        normed = rms_norm(hidden, norm_w)
        q_rot = apply_rotary(project(normed, w_q, b_q).reshape(n_rows, 24, D), positions)
        k_rot = apply_rotary(project(normed, w_k, b_k).reshape(n_rows, 1, D), positions)
        v_new = project(normed, w_v, b_v).reshape(n_rows, 1, D)
        q_pad = jnp.pad(q_rot.reshape(n_rows, 2, HALF, D), ((0, 0), (0, 0), (0, SLOT - HALF), (0, 0)))
        q_pad = q_pad.reshape(n_rows, 2 * SLOT, D)
        y_out = tail(q_pad, k_rot.astype(F32), v_new.astype(F32), seq_lens, hidden,
                     k_cache.reshape(n_rows, S_DEV, D), v_cache.reshape(n_rows, S_DEV, D), w_o)
        return y_out, k_rot, v_new

    col_spec = P(None, 'tp')
    vec_spec = P('tp')
    cache_spec = P('dp', 'sp', 'tp', None)
    group_spec = P('dp', 'tp', None)
    in_specs = (P('dp', None), P(None), col_spec, vec_spec, col_spec, vec_spec, col_spec, vec_spec,
                P('tp', None), cache_spec, cache_spec, P('dp'), P('dp'))
    out_specs = (P('dp', None), group_spec, group_spec)
    return jax.shard_map(device_step, mesh=mesh, in_specs=in_specs, out_specs=out_specs, check_vma=False)
```

```python
import functools
import math

import jax
import jax.numpy as jnp
from jax import lax
from jax.experimental import pallas as pl
from jax.experimental.pallas import tpu as pltpu
from jax.sharding import PartitionSpec as P

RMS_EPS = 1.5625e-7
ROPE_BASE = 10000.0
NEG_BIG = -3.0e38
MESH = pl.DeviceIdType.MESH
F32 = jnp.float32
BF16 = jnp.bfloat16

N_ROWS = 32
S_DEV = 512
D = 128
SP = 64
PLANE = 16
HALF = 12
SLOT = 16
N_OUT = 6144
N_Z = 1536
AG = 24
UNROLL = 8
Q_DEV = 384
K_CUT = 1536


def step_kernel(hid_hbm, nw_ref, bq_ref, bk_ref, bv_ref, freq_ref, pos_ref, seq_ref,
                wq_hbm, wk_hbm, wv_hbm, k_hbm, v_hbm, wo_hbm, y_ref, kn_ref, vn_ref,
                hid_ref, normed, wqbuf, wkvbuf, q_all, kn_rows, vn_rows,
                kbuf, vbuf, wobuf, o_send, o_recv, a_all, lhs, ypart, yrecv, ag,
                hsem, wqsem, wkvsem, q_send, q_recv,
                ksem, vsem, wsem, rs_send, rs_recv, z_send, z_recv, d_send, d_recv,
                ag_send, ag_recv, f_send, f_recv):
    c = lax.axis_index('tp')
    s = lax.axis_index('sp')
    z = lax.div(s, PLANE)
    p = lax.rem(s, PLANE)
    y_at = lax.div(p, 4)
    x_at = lax.rem(p, 4)
    qk_scale = (D ** -0.5) * math.log2(math.e)

    def chip_of(i):
        return lax.rem(p + 1 + lax.div(i, 2), PLANE)

    def row_of(i):
        return chip_of(i) + PLANE * lax.rem(i, 2)

    label = 4 * lax.rem(z, 2) + 2 * lax.rem(y_at, 2) + lax.rem(x_at, 2)
    hid_copy = pltpu.make_async_copy(hid_hbm, hid_ref, hsem)
    hid_copy.start()
    q_cols = pl.ds(pl.multiple_of(label * Q_DEV, D), Q_DEV)
    wq_copies = [pltpu.make_async_copy(
        wq_hbm.at[pl.ds(K_CUT * j, K_CUT), q_cols], wqbuf.at[pl.ds(K_CUT * j, K_CUT)], wqsem.at[j])
        for j in range(N_OUT // K_CUT)]
    for cp in wq_copies:
        cp.start()

    barrier = pltpu.get_barrier_semaphore()

    def greet(d, carry):
        pl.semaphore_signal(barrier, inc=1, device_id={'sp': lax.rem(s + d, SP)}, device_id_type=MESH)
        return carry
    lax.fori_loop(1, SP, greet, 0)
    pl.semaphore_signal(barrier, inc=1, device_id={'tp': 1 - c}, device_id_type=MESH)

    wkv_copies = [pltpu.make_async_copy(wk_hbm, wkvbuf.at[:, pl.ds(0, D)], wkvsem.at[0]),
                  pltpu.make_async_copy(wv_hbm, wkvbuf.at[:, pl.ds(D, D)], wkvsem.at[1])]
    for cp in wkv_copies:
        cp.start()

    def k_copy(i):
        return pltpu.make_async_copy(k_hbm.at[row_of(i)], kbuf.at[i], ksem.at[i])

    def v_copy(i):
        return pltpu.make_async_copy(v_hbm.at[row_of(i)], vbuf.at[i], vsem.at[i])

    def start_kv(i, carry):
        k_copy(i).start()
        v_copy(i).start()
        return carry
    wo_copies = [pltpu.make_async_copy(
        wo_hbm.at[pl.ds(768 * j, 768), pl.ds(pl.multiple_of(z * N_Z, N_Z), N_Z)],
        wobuf.at[pl.ds(768 * j, 768)], wsem.at[j]) for j in range(4)]

    row_eye = lax.broadcasted_iota(jnp.int32, (N_ROWS, N_ROWS), 0) == lax.broadcasted_iota(jnp.int32, (N_ROWS, N_ROWS), 1)
    pos_col = jnp.sum(jnp.where(row_eye, pos_ref[...].astype(F32), 0.0), axis=1, keepdims=True)
    angles = pos_col * freq_ref[...]
    is_even = lax.rem(lax.broadcasted_iota(jnp.int32, (N_ROWS, D), 1), 2) == 0
    cos_t = jnp.cos(angles)
    sin_t = jnp.where(is_even, -jnp.sin(angles), jnp.sin(angles))

    def rotate(head):
        other = jnp.where(is_even, pltpu.roll(head, D - 1, 1), pltpu.roll(head, 1, 1))
        return (head * cos_t + other * sin_t).astype(BF16)

    hid_copy.wait()
    x_f32 = hid_ref[...].astype(F32)
    mean_sq = jnp.mean(x_f32 * x_f32, axis=-1, keepdims=True)
    normed[...] = (x_f32 * lax.rsqrt(mean_sq + RMS_EPS) * nw_ref[...].astype(F32)).astype(BF16)

    q_mine = jnp.zeros((N_ROWS, Q_DEV), F32)
    for j, cp in enumerate(wq_copies):
        cp.wait()
        cut = slice(K_CUT * j, K_CUT * (j + 1))
        q_mine = q_mine + jnp.dot(normed[:, cut], wqbuf[cut, :], preferred_element_type=F32)
    lax.fori_loop(0, N_ROWS, start_kv, 0)
    for cp in wo_copies:
        cp.start()
    bias = jnp.zeros((1, Q_DEV), F32)
    for j in range(8):
        bias = jnp.where(label == j, bq_ref[:, j * Q_DEV:(j + 1) * Q_DEV].astype(F32), bias)
    q_mine = (q_mine + bias).astype(BF16).astype(F32)
    for hf in range(2):
        q_all[pl.ds((hf * SLOT + HALF) * N_ROWS, (SLOT - HALF) * N_ROWS), :] = jnp.zeros(((SLOT - HALF) * N_ROWS, D), F32)

    def q_rows(lab):
        first = lax.div(lab, 4) * SLOT + 3 * lax.rem(lab, 4)
        return pl.multiple_of(first * N_ROWS, N_ROWS)
    for t in range(3):
        q_all[pl.ds(q_rows(label) + t * N_ROWS, N_ROWS), :] = rotate(q_mine[:, t * D:(t + 1) * D]).astype(F32)

    pl.semaphore_wait(barrier, SP)

    def across(v):
        return lax.rem(v + 4 + (1 - 2 * lax.rem(v, 2)) * (1 - 2 * c), 4)
    q_copies = []
    for mask in range(7, 0, -1):
        zd = across(z) if mask & 4 else z
        yd = across(y_at) if mask & 2 else y_at
        xd = across(x_at) if mask & 1 else x_at
        mine = q_all.at[pl.ds(q_rows(label), 3 * N_ROWS)]
        q_copies.append(pltpu.make_async_remote_copy(
            src_ref=mine, dst_ref=mine, send_sem=q_send.at[mask - 1], recv_sem=q_recv.at[mask - 1],
            device_id={'sp': zd * PLANE + yd * 4 + xd}, device_id_type=MESH))
    for cp in q_copies:
        cp.start()

    for cp in wkv_copies:
        cp.wait()
    kv = jnp.dot(normed[...], wkvbuf[...], preferred_element_type=F32)
    k_new = rotate((kv[:, :D] + bk_ref[...].astype(F32)).astype(BF16).astype(F32))
    v_new = (kv[:, D:] + bv_ref[...].astype(F32)).astype(BF16)
    kn_ref[...] = k_new
    vn_ref[...] = v_new
    kn_rows[...] = k_new.astype(F32)
    vn_rows[...] = v_new.astype(F32)
    for cp in q_copies:
        cp.wait_recv()

    lane = lax.broadcasted_iota(jnp.int32, (SLOT, D), 1)
    sub = lax.broadcasted_iota(jnp.int32, (SLOT, D), 0)
    eye = lane == sub
    pos = s * S_DEV + lax.broadcasted_iota(jnp.int32, (2 * SLOT, S_DEV), 1)

    def rs_copy(i, hf):
        dest = (2 * lax.rem(i, 2) + hf) * PLANE + chip_of(i)
        slot = 2 * i + hf
        return dest, pltpu.make_async_remote_copy(
            src_ref=o_send.at[slot], dst_ref=o_recv.at[pl.ds(pl.multiple_of(s * SLOT, SLOT), SLOT)],
            send_sem=rs_send, recv_sem=rs_recv, device_id={'sp': dest}, device_id_type=MESH)

    def rows_step(g, carry):
        idx = [g * UNROLL + u for u in range(UNROLL)]
        rows = [row_of(i) for i in idx]
        scores = []
        for i, b in zip(idx, rows):
            k_copy(i).wait()
            sc = lax.dot_general(q_all[pl.ds(b, 2 * SLOT, stride=N_ROWS), :].astype(BF16), kbuf[i], (((1,), (1,)), ((), ())), preferred_element_type=F32)
            scores.append(jnp.where(pos < seq_ref[b], sc, NEG_BIG))
        tops = [jnp.max(sc, axis=1, keepdims=True) for sc in scores]
        probs = [jnp.exp2((sc - m) * qk_scale) for sc, m in zip(scores, tops)]
        sums = [jnp.sum(pr, axis=1, keepdims=True) for pr in probs]
        for i, m, l, pr in zip(idx, tops, sums, probs):
            v_copy(i).wait()
            o = jnp.dot(pr.astype(BF16), vbuf[i], preferred_element_type=F32)
            m2 = m * qk_scale
            for hf in range(2):
                part = slice(hf * SLOT, (hf + 1) * SLOT)
                m_row = jnp.sum(jnp.where(eye, m2[part], 0.0), axis=0, keepdims=True)
                l_row = jnp.sum(jnp.where(eye, l[part], 0.0), axis=0, keepdims=True)
                o_send[2 * i + hf] = jnp.where(sub == HALF, m_row, jnp.where(sub == HALF + 1, l_row, o[part]))
        for i in idx:
            for hf in range(2):
                dest, cp = rs_copy(i, hf)

                @pl.when(dest != s)
                def _():
                    cp.start()

                @pl.when(dest == s)
                def _():
                    o_recv[pl.ds(pl.multiple_of(s * SLOT, SLOT), SLOT), :] = o_send[2 * i + hf]
        return carry
    lax.fori_loop(0, N_ROWS // UNROLL, rows_step, 0)

    my_row = p + PLANE * lax.div(z, 2)
    my_half = lax.rem(z, 2)
    q_own = q_all[pl.ds(my_half * SLOT * N_ROWS + my_row, SLOT, stride=N_ROWS), :]
    k_mine = kn_rows[pl.ds(my_row, 1), :]
    v_mine = vn_rows[pl.ds(my_row, 1), :]
    s_new = jnp.sum(q_own * k_mine, axis=1, keepdims=True) * qk_scale

    def all_in(ref, sem):
        pltpu.make_async_copy(ref, ref, sem).wait()

    all_in(o_recv.at[pl.ds(0, (SP - 1) * SLOT)], rs_recv)
    m_rows = o_recv[pl.ds(HALF, SP, stride=SLOT), :]
    l_rows = o_recv[pl.ds(HALF + 1, SP, stride=SLOT), :]
    stats = jnp.transpose(jnp.concatenate([m_rows, l_rows], axis=0))[:SLOT]
    m_cols, l_cols = stats[:, :SP], stats[:, SP:]
    m_top = jnp.maximum(jnp.max(m_cols, axis=1, keepdims=True), s_new)
    w_cols = jnp.exp2(m_cols - m_top)
    w_new = jnp.exp2(s_new - m_top)
    l_all = jnp.sum(w_cols * l_cols, axis=1, keepdims=True) + w_new
    acc = w_new * v_mine
    for j in range(SP):
        acc = acc + w_cols[:, j:j + 1] * o_recv[j * SLOT:(j + 1) * SLOT, :]
    a_all[z] = acc / l_all

    z_copies = []
    for dz in range(1, 4):
        z_copies.append(pltpu.make_async_remote_copy(
            src_ref=a_all.at[z], dst_ref=a_all.at[z], send_sem=z_send.at[dz - 1], recv_sem=z_recv.at[dz - 1],
            device_id={'sp': lax.rem(z + dz, 4) * PLANE + p}, device_id_type=MESH))
    for cp in z_copies:
        cp.start()
    lhs[...] = jnp.zeros_like(lhs)
    for cp in z_copies:
        cp.wait_recv()
    for zz in range(4):
        r, hf = zz // 2, zz % 2
        for j in range(HALF):
            lhs[r:r + 1, (hf * HALF + j) * D:(hf * HALF + j + 1) * D] = a_all[zz, j:j + 1, :]
    for cp in wo_copies:
        cp.wait()
    ypart[0] = jnp.dot(lhs[...].astype(BF16), wobuf[...], preferred_element_type=F32)

    d_copy = pltpu.make_async_remote_copy(
        src_ref=ypart.at[0], dst_ref=ypart.at[1], send_sem=d_send, recv_sem=d_recv,
        device_id={'tp': 1 - c}, device_id_type=MESH)
    d_copy.start()
    d_copy.wait_recv()
    both = ypart[0] + ypart[1]

    def ag_slot(i):
        return ag.at[pl.ds(pl.multiple_of(i * AG, 8), AG)]

    for r in range(2):
        for blk in range(12):
            yrecv[r * 12 + blk:r * 12 + blk + 1, :] = both[r:r + 1, blk * D:(blk + 1) * D]
    ag[pl.ds(pl.multiple_of(s * AG, 8), AG), :] = yrecv[...]
    par = lax.rem(s + c, 2)

    def ag_copy(i):
        dest = 2 * i + par
        return dest, pltpu.make_async_remote_copy(
            src_ref=ag_slot(s), dst_ref=ag_slot(s), send_sem=ag_send.at[i], recv_sem=ag_recv.at[lax.div(s, 2)],
            device_id={'sp': dest}, device_id_type=MESH)

    def ag_start(i, carry):
        dest, cp = ag_copy(i)

        @pl.when(dest != s)
        def _():
            cp.start()
        return carry
    lax.fori_loop(0, SP // 2, ag_start, 0)

    def forward(i):
        return pltpu.make_async_remote_copy(
            src_ref=ag_slot(2 * i + par), dst_ref=ag_slot(2 * i + par), send_sem=f_send.at[i], recv_sem=f_recv.at[i],
            device_id={'tp': 1 - c}, device_id_type=MESH)

    def relay(i, carry):
        src = 2 * i + par

        @pl.when(src != s)
        def _():
            pltpu.make_async_copy(ag_slot(src), ag_slot(src), ag_recv.at[i]).wait()
            forward(i).start()
        return carry
    lax.fori_loop(0, SP // 2, relay, 0)

    def relayed(i, carry):
        src = 2 * i + 1 - par

        @pl.when(src != s)
        def _():
            pltpu.make_async_copy(ag_slot(src), ag_slot(src), f_recv.at[i]).wait()
        return carry
    lax.fori_loop(0, SP // 2, relayed, 0)

    for zz in range(4):
        for blk in range(12):
            col = slice(zz * N_Z + blk * D, zz * N_Z + (blk + 1) * D)
            for r in range(2):
                rows = slice(PLANE * r, PLANE * (r + 1))
                y_blk = ag[pl.ds(zz * PLANE * AG + r * 12 + blk, PLANE, stride=AG), :]
                y_ref[rows, col] = (hid_ref[rows, col].astype(F32) + y_blk).astype(BF16)

    all_in(o_send.at[pl.ds(0, SP - 1)], rs_send)
    for cp in q_copies + z_copies:
        cp.wait_send()
    d_copy.wait_send()

    def drain(i, carry):
        dest, cp = ag_copy(i)

        @pl.when(dest != s)
        def _():
            cp.wait_send()

        @pl.when(2 * i + par != s)
        def _():
            forward(i).wait_send()
        return carry
    lax.fori_loop(0, SP // 2, drain, 0)


def step_call(freq, *operands):
    hidden, norm_w, w_q, b_q, w_k, b_k, w_v, b_v, w_o, k_cache, v_cache, positions, seq_lens = operands
    vmem = pl.BlockSpec(memory_space=pltpu.VMEM)
    smem = pl.BlockSpec(memory_space=pltpu.SMEM)
    hbm = pl.BlockSpec(memory_space=pl.ANY)
    dma = pltpu.SemaphoreType.DMA
    return pl.pallas_call(
        step_kernel,
        out_shape=(jax.ShapeDtypeStruct((N_ROWS, N_OUT), BF16),
                   jax.ShapeDtypeStruct((N_ROWS, D), BF16), jax.ShapeDtypeStruct((N_ROWS, D), BF16)),
        in_specs=[hbm, vmem, vmem, vmem, vmem, vmem, vmem, smem, hbm, hbm, hbm, hbm, hbm, hbm],
        out_specs=(vmem, vmem, vmem),
        scratch_shapes=[
            pltpu.VMEM((N_ROWS, N_OUT), BF16),
            pltpu.VMEM((N_ROWS, N_OUT), BF16),
            pltpu.VMEM((N_OUT, Q_DEV), BF16),
            pltpu.VMEM((N_OUT, 2 * D), BF16),
            pltpu.VMEM((2 * SLOT * N_ROWS, D), F32),
            pltpu.VMEM((N_ROWS, D), F32),
            pltpu.VMEM((N_ROWS, D), F32),
            pltpu.VMEM((N_ROWS, S_DEV, D), BF16),
            pltpu.VMEM((N_ROWS, S_DEV, D), BF16),
            pltpu.VMEM((3072, N_Z), BF16),
            pltpu.VMEM((2 * N_ROWS, SLOT, D), F32),
            pltpu.VMEM((SP * SLOT, D), F32),
            pltpu.VMEM((4, SLOT, D), F32),
            pltpu.VMEM((8, 3072), F32),
            pltpu.VMEM((2, 8, N_Z), F32),
            pltpu.VMEM((AG, D), F32),
            pltpu.VMEM((SP * AG, D), F32),
            dma, dma((N_OUT // K_CUT,)), dma((2,)), dma((7,)), dma((7,)),
            dma((N_ROWS,)), dma((N_ROWS,)), dma((4,)),
            dma, dma, dma((3,)), dma((3,)), dma, dma,
            dma((SP // 2,)), dma((SP // 2,)), dma((SP // 2,)), dma((SP // 2,)),
        ],
        compiler_params=pltpu.CompilerParams(
            collective_id=0, has_side_effects=True, vmem_limit_bytes=56 * 1024 * 1024),
        name='decode_step',
    )(hidden, norm_w.reshape(1, -1), b_q.reshape(1, -1), b_k.reshape(1, -1), b_v.reshape(1, -1), freq,
      positions.reshape(1, -1), seq_lens, w_q, w_k, w_v,
      k_cache.reshape(N_ROWS, S_DEV, D), v_cache.reshape(N_ROWS, S_DEV, D), w_o)


def solution(mesh):
    def device_step(*operands):
        inv_freq = ROPE_BASE ** (-2.0 * jnp.arange(D // 4, dtype=jnp.float32) / (D // 2))
        freq = jnp.pad(jnp.repeat(inv_freq, 2), (0, D // 2)).reshape(1, D)
        y_out, k_new, v_new = step_call(freq, *operands)
        return y_out, k_new.reshape(N_ROWS, 1, D), v_new.reshape(N_ROWS, 1, D)

    col_spec = P(None, 'tp')
    vec_spec = P('tp')
    cache_spec = P('dp', 'sp', 'tp', None)
    group_spec = P('dp', 'tp', None)
    in_specs = (P('dp', None), P(None), col_spec, vec_spec, col_spec, vec_spec, col_spec, vec_spec,
                P('tp', None), cache_spec, cache_spec, P('dp'), P('dp'))
    out_specs = (P('dp', None), group_spec, group_spec)
    return jax.shard_map(device_step, mesh=mesh, in_specs=in_specs, out_specs=out_specs, check_vma=False)
```

```python
import functools
import math

import jax
import jax.numpy as jnp
from jax import lax
from jax.experimental import pallas as pl
from jax.experimental.pallas import tpu as pltpu
from jax.sharding import PartitionSpec as P

RMS_EPS = 1.5625e-7
ROPE_BASE = 10000.0
NEG_BIG = -3.0e38
MESH = pl.DeviceIdType.MESH
F32 = jnp.float32
BF16 = jnp.bfloat16

N_ROWS = 32
S_DEV = 512
D = 128
SP = 64
PLANE = 16
HALF = 12
SLOT = 16
N_OUT = 6144
N_Z = 1536
AG = 24
Q_DEV = 384
K_CUT = 1536


def step_kernel(hid_hbm, nw_hbm, bq_hbm, bk_hbm, bv_hbm, freq_ref, pos_hbm, seq_hbm,
                wq_hbm, wk_hbm, wv_hbm, k_hbm, v_hbm, wo_hbm, ag, kn_rows, vn_rows,
                nw_ref, bq_ref, bk_ref, bv_ref, pos_ref, seq_ref, hid_ref, normed, wqbuf, wkvbuf, bq_rows, q_all,
                kbuf, vbuf, wobuf, o_send, o_recv, a_all, lhs, ypart, yrecv,
                vecsem, hsem, wqsem, wkvsem, q_send, q_recv,
                ksem, vsem, wsem, rs_send, rs_recv, z_send, z_recv, d_send, d_recv,
                ag_send, ag_recv, f_send, f_recv):
    c = lax.axis_index('tp')
    s = lax.axis_index('sp')
    z = lax.div(s, PLANE)
    p = lax.rem(s, PLANE)
    y_at = lax.div(p, 4)
    x_at = lax.rem(p, 4)
    qk_scale = (D ** -0.5) * math.log2(math.e)

    label = 4 * lax.rem(z, 2) + 2 * lax.rem(y_at, 2) + lax.rem(x_at, 2)
    hid_copy = pltpu.make_async_copy(hid_hbm, hid_ref, hsem)
    hid_copy.start()
    vec_copies = [pltpu.make_async_copy(src, dst, vecsem.at[j]) for j, (src, dst) in enumerate((
        (pos_hbm, pos_ref), (nw_hbm, nw_ref), (bq_hbm, bq_ref), (bk_hbm, bk_ref), (bv_hbm, bv_ref), (seq_hbm, seq_ref)))]
    for cp in vec_copies:
        cp.start()
    q_cols = pl.ds(pl.multiple_of(label * Q_DEV, D), Q_DEV)
    wq_copies = [pltpu.make_async_copy(
        wq_hbm.at[pl.ds(K_CUT * j, K_CUT), q_cols], wqbuf.at[pl.ds(K_CUT * j, K_CUT)], wqsem.at[j])
        for j in range(N_OUT // K_CUT)]
    for cp in wq_copies:
        cp.start()

    barrier = pltpu.get_barrier_semaphore()

    def greet(d, carry):
        pl.semaphore_signal(barrier, inc=1, device_id={'sp': lax.rem(s + d, SP)}, device_id_type=MESH)
        return carry
    lax.fori_loop(1, SP, greet, 0)
    pl.semaphore_signal(barrier, inc=1, device_id={'tp': 1 - c}, device_id_type=MESH)

    wkv_copies = [pltpu.make_async_copy(wk_hbm, wkvbuf.at[:, pl.ds(0, D)], wkvsem.at[0]),
                  pltpu.make_async_copy(wv_hbm, wkvbuf.at[:, pl.ds(D, D)], wkvsem.at[1])]
    for cp in wkv_copies:
        cp.start()

    def kv_copies(step):
        y_to = lax.rem(y_at + 1 + step, 4)
        pairs = []
        for r in range(2):
            rows = pl.ds(PLANE * r + 4 * y_to, 4)
            pairs.append(pltpu.make_async_copy(k_hbm.at[rows], kbuf.at[rows], ksem.at[2 * step + r]))
            pairs.append(pltpu.make_async_copy(v_hbm.at[rows], vbuf.at[rows], vsem.at[2 * step + r]))
        return pairs
    wo_copies = [pltpu.make_async_copy(
        wo_hbm.at[pl.ds(768 * j, 768), pl.ds(pl.multiple_of(z * N_Z, N_Z), N_Z)],
        wobuf.at[pl.ds(768 * j, 768)], wsem.at[j]) for j in range(4)]

    vec_copies[0].wait()
    row_eye = lax.broadcasted_iota(jnp.int32, (N_ROWS, N_ROWS), 0) == lax.broadcasted_iota(jnp.int32, (N_ROWS, N_ROWS), 1)
    pos_col = jnp.sum(jnp.where(row_eye, pos_ref[...].astype(F32), 0.0), axis=1, keepdims=True)
    angles = pos_col * freq_ref[...]
    is_even = lax.rem(lax.broadcasted_iota(jnp.int32, (N_ROWS, D), 1), 2) == 0
    cos_t = jnp.cos(angles)
    sin_t = jnp.where(is_even, -jnp.sin(angles), jnp.sin(angles))

    def rotate(head):
        other = jnp.where(is_even, pltpu.roll(head, D - 1, 1), pltpu.roll(head, 1, 1))
        return (head * cos_t + other * sin_t).astype(BF16)

    hid_copy.wait()
    for cp in vec_copies[1:]:
        cp.wait()
    x_f32 = hid_ref[...].astype(F32)
    mean_sq = jnp.mean(x_f32 * x_f32, axis=-1, keepdims=True)
    unit = lax.rsqrt(mean_sq + RMS_EPS)
    nw_rows = nw_ref[...].astype(F32)
    for j in range(N_OUT // D):
        cut = slice(j * D, (j + 1) * D)
        normed[:, cut] = (x_f32[:, cut] * unit * nw_rows[j:j + 1, :]).astype(BF16)
    bq_rows[...] = bq_ref[...].astype(F32)

    q_mine = jnp.zeros((N_ROWS, Q_DEV), F32)
    for j, cp in enumerate(wq_copies):
        cp.wait()
        cut = slice(K_CUT * j, K_CUT * (j + 1))
        q_mine = q_mine + jnp.dot(normed[:, cut], wqbuf[cut, :], preferred_element_type=F32)
    for step in range(4):
        for cp in kv_copies(step):
            cp.start()
    for cp in wo_copies:
        cp.start()
    for hf in range(2):
        q_all[pl.ds((hf * SLOT + HALF) * N_ROWS, (SLOT - HALF) * N_ROWS), :] = jnp.zeros(((SLOT - HALF) * N_ROWS, D), F32)

    def q_rows(lab):
        first = lax.div(lab, 4) * SLOT + 3 * lax.rem(lab, 4)
        return pl.multiple_of(first * N_ROWS, N_ROWS)
    for t in range(3):
        head = q_mine[:, t * D:(t + 1) * D] + bq_rows[pl.ds(3 * label + t, 1), :]
        q_all[pl.ds(q_rows(label) + t * N_ROWS, N_ROWS), :] = rotate(head.astype(BF16).astype(F32)).astype(F32)

    pl.semaphore_wait(barrier, SP)

    def across(v):
        return lax.rem(v + 4 + (1 - 2 * lax.rem(v, 2)) * (1 - 2 * c), 4)
    q_copies = []
    for mask in range(7, 0, -1):
        zd = across(z) if mask & 4 else z
        yd = across(y_at) if mask & 2 else y_at
        xd = across(x_at) if mask & 1 else x_at
        mine = q_all.at[pl.ds(q_rows(label), 3 * N_ROWS)]
        q_copies.append(pltpu.make_async_remote_copy(
            src_ref=mine, dst_ref=mine, send_sem=q_send.at[mask - 1], recv_sem=q_recv.at[mask - 1],
            device_id={'sp': zd * PLANE + yd * 4 + xd}, device_id_type=MESH))
    for cp in q_copies:
        cp.start()

    for cp in wkv_copies:
        cp.wait()
    kv = jnp.dot(normed[...], wkvbuf[...], preferred_element_type=F32)
    k_new = rotate((kv[:, :D] + bk_ref[...].astype(F32)).astype(BF16).astype(F32))
    v_new = (kv[:, D:] + bv_ref[...].astype(F32)).astype(BF16)
    kn_rows[...] = k_new.astype(F32)
    vn_rows[...] = v_new.astype(F32)
    for cp in q_copies:
        cp.wait_recv()

    lane = lax.broadcasted_iota(jnp.int32, (SLOT, D), 1)
    sub = lax.broadcasted_iota(jnp.int32, (SLOT, D), 0)
    eye = lane == sub
    pos = s * S_DEV + lax.broadcasted_iota(jnp.int32, (2 * SLOT, S_DEV), 1)

    def rs_copy(dest):
        return pltpu.make_async_remote_copy(
            src_ref=o_send.at[dest], dst_ref=o_recv.at[pl.ds(pl.multiple_of(s * SLOT, SLOT), SLOT)],
            send_sem=rs_send, recv_sem=rs_recv, device_id={'sp': dest}, device_id_type=MESH)

    def rows_step(step, carry):
        y_to = lax.rem(y_at + 1 + step, 4)
        for cp in kv_copies(step):
            cp.wait()
        work = []
        for u in range(4):
            for r in range(2):
                chip = 4 * y_to + lax.rem(x_at + 1 + u, 4)
                work.append((u, r, chip, chip + PLANE * r))
        scores = []
        for u, r, chip, b in work:
            sc = lax.dot_general(q_all[pl.ds(b, 2 * SLOT, stride=N_ROWS), :].astype(BF16), kbuf[b],
                                 (((1,), (1,)), ((), ())), preferred_element_type=F32)
            scores.append(jnp.where(pos < seq_ref[b], sc, NEG_BIG))
        tops = [jnp.max(sc, axis=1, keepdims=True) for sc in scores]
        probs = [jnp.exp2((sc - m) * qk_scale) for sc, m in zip(scores, tops)]
        sums = [jnp.sum(pr, axis=1, keepdims=True) for pr in probs]
        for (u, r, chip, b), m, l, pr in zip(work, tops, sums, probs):
            o = jnp.dot(pr.astype(BF16), vbuf[b], preferred_element_type=F32)
            m2 = m * qk_scale
            for hf in range(2):
                part = slice(hf * SLOT, (hf + 1) * SLOT)
                m_row = jnp.sum(jnp.where(eye, m2[part], 0.0), axis=0, keepdims=True)
                l_row = jnp.sum(jnp.where(eye, l[part], 0.0), axis=0, keepdims=True)
                o_send[(2 * r + hf) * PLANE + chip] = jnp.where(
                    sub == HALF, m_row, jnp.where(sub == HALF + 1, l_row, o[part]))
        for u, r, chip, b in work:
            for hf in range(2):
                dest = (2 * r + hf) * PLANE + chip
                if u < 3:
                    rs_copy(dest).start()
                else:
                    @pl.when(dest != s)
                    def _():
                        rs_copy(dest).start()
        return carry
    lax.fori_loop(0, 4, rows_step, 0)
    mine = pl.ds(pl.multiple_of(s * SLOT, SLOT), SLOT)
    o_recv[mine, :] = o_send[s]

    my_row = p + PLANE * lax.div(z, 2)
    my_half = lax.rem(z, 2)
    q_own = q_all[pl.ds(my_half * SLOT * N_ROWS + my_row, SLOT, stride=N_ROWS), :]
    k_mine = kn_rows[pl.ds(my_row, 1), :]
    v_mine = vn_rows[pl.ds(my_row, 1), :]
    s_new = jnp.sum(q_own * k_mine, axis=1, keepdims=True) * qk_scale

    def all_in(ref, sem):
        pltpu.make_async_copy(ref, ref, sem).wait()

    all_in(o_recv.at[pl.ds(0, (SP - 1) * SLOT)], rs_recv)
    m_rows = o_recv[pl.ds(HALF, SP, stride=SLOT), :]
    l_rows = o_recv[pl.ds(HALF + 1, SP, stride=SLOT), :]
    stats = jnp.transpose(jnp.concatenate([m_rows, l_rows], axis=0))[:SLOT]
    m_cols, l_cols = stats[:, :SP], stats[:, SP:]
    m_top = jnp.maximum(jnp.max(m_cols, axis=1, keepdims=True), s_new)
    w_cols = jnp.exp2(m_cols - m_top)
    w_new = jnp.exp2(s_new - m_top)
    l_all = jnp.sum(w_cols * l_cols, axis=1, keepdims=True) + w_new
    acc = w_new * v_mine
    for j in range(SP):
        acc = acc + w_cols[:, j:j + 1] * o_recv[j * SLOT:(j + 1) * SLOT, :]
    a_all[z] = acc / l_all

    z_copies = []
    for dz in range(1, 4):
        z_copies.append(pltpu.make_async_remote_copy(
            src_ref=a_all.at[z], dst_ref=a_all.at[z], send_sem=z_send.at[dz - 1], recv_sem=z_recv.at[dz - 1],
            device_id={'sp': lax.rem(z + dz, 4) * PLANE + p}, device_id_type=MESH))
    for cp in z_copies:
        cp.start()
    lhs[...] = jnp.zeros_like(lhs)
    for cp in z_copies:
        cp.wait_recv()
    for zz in range(4):
        r, hf = zz // 2, zz % 2
        for j in range(HALF):
            lhs[r:r + 1, (hf * HALF + j) * D:(hf * HALF + j + 1) * D] = a_all[zz, j:j + 1, :]
    for cp in wo_copies:
        cp.wait()
    ypart[0] = jnp.dot(lhs[...].astype(BF16), wobuf[...], preferred_element_type=F32)

    d_copy = pltpu.make_async_remote_copy(
        src_ref=ypart.at[0], dst_ref=ypart.at[1], send_sem=d_send, recv_sem=d_recv,
        device_id={'tp': 1 - c}, device_id_type=MESH)
    d_copy.start()
    d_copy.wait_recv()
    both = ypart[0] + ypart[1]

    def ag_slot(i):
        return ag.at[pl.ds(pl.multiple_of(i * AG, 8), AG)]

    for r in range(2):
        for blk in range(12):
            yrecv[r * 12 + blk:r * 12 + blk + 1, :] = both[r:r + 1, blk * D:(blk + 1) * D]
    ag[pl.ds(pl.multiple_of(s * AG, 8), AG), :] = yrecv[...]
    par = lax.rem(s + c, 2)

    def ag_copy(i):
        dest = 2 * i + par
        return dest, pltpu.make_async_remote_copy(
            src_ref=ag_slot(s), dst_ref=ag_slot(s), send_sem=ag_send.at[i], recv_sem=ag_recv.at[lax.div(s, 2)],
            device_id={'sp': dest}, device_id_type=MESH)

    def ag_start(i, carry):
        dest, cp = ag_copy(i)

        @pl.when(dest != s)
        def _():
            cp.start()
        return carry
    lax.fori_loop(0, SP // 2, ag_start, 0)

    def forward(i):
        return pltpu.make_async_remote_copy(
            src_ref=ag_slot(2 * i + par), dst_ref=ag_slot(2 * i + par), send_sem=f_send.at[i], recv_sem=f_recv.at[i],
            device_id={'tp': 1 - c}, device_id_type=MESH)

    def relay(i, carry):
        src = 2 * i + par

        @pl.when(src != s)
        def _():
            pltpu.make_async_copy(ag_slot(src), ag_slot(src), ag_recv.at[i]).wait()
            forward(i).start()
        return carry
    lax.fori_loop(0, SP // 2, relay, 0)

    def relayed(i, carry):
        src = 2 * i + 1 - par

        @pl.when(src != s)
        def _():
            pltpu.make_async_copy(ag_slot(src), ag_slot(src), f_recv.at[i]).wait()
        return carry
    lax.fori_loop(0, SP // 2, relayed, 0)

    all_in(o_send.at[pl.ds(0, SP - 1)], rs_send)
    for cp in q_copies + z_copies:
        cp.wait_send()
    d_copy.wait_send()

    def drain(i, carry):
        dest, cp = ag_copy(i)

        @pl.when(dest != s)
        def _():
            cp.wait_send()

        @pl.when(2 * i + par != s)
        def _():
            forward(i).wait_send()
        return carry
    lax.fori_loop(0, SP // 2, drain, 0)


def step_call(freq, *operands):
    hidden, norm_w, w_q, b_q, w_k, b_k, w_v, b_v, w_o, k_cache, v_cache, positions, seq_lens = operands
    vmem = pl.BlockSpec(memory_space=pltpu.VMEM)
    hbm = pl.BlockSpec(memory_space=pltpu.HBM)
    dma = pltpu.SemaphoreType.DMA
    return pl.pallas_call(
        step_kernel,
        out_shape=(jax.ShapeDtypeStruct((SP * AG, D), F32),
                   jax.ShapeDtypeStruct((N_ROWS, D), F32), jax.ShapeDtypeStruct((N_ROWS, D), F32)),
        in_specs=[hbm, hbm, hbm, hbm, hbm, vmem, hbm, hbm, hbm, hbm, hbm, hbm, hbm, hbm],
        out_specs=(vmem, vmem, vmem),
        scratch_shapes=[
            pltpu.VMEM((N_OUT // D, D), BF16),
            pltpu.VMEM((24, D), BF16),
            pltpu.VMEM((1, D), BF16),
            pltpu.VMEM((1, D), BF16),
            pltpu.VMEM((1, N_ROWS), jnp.int32),
            pltpu.SMEM((N_ROWS,), jnp.int32),
            pltpu.VMEM((N_ROWS, N_OUT), BF16),
            pltpu.VMEM((N_ROWS, N_OUT), BF16),
            pltpu.VMEM((N_OUT, Q_DEV), BF16),
            pltpu.VMEM((N_OUT, 2 * D), BF16),
            pltpu.VMEM((24, D), F32),
            pltpu.VMEM((2 * SLOT * N_ROWS, D), F32),
            pltpu.VMEM((N_ROWS, S_DEV, D), BF16),
            pltpu.VMEM((N_ROWS, S_DEV, D), BF16),
            pltpu.VMEM((3072, N_Z), BF16),
            pltpu.VMEM((2 * N_ROWS, SLOT, D), F32),
            pltpu.VMEM((SP * SLOT, D), F32),
            pltpu.VMEM((4, SLOT, D), F32),
            pltpu.VMEM((8, 3072), F32),
            pltpu.VMEM((2, 8, N_Z), F32),
            pltpu.VMEM((AG, D), F32),
            dma((6,)), dma, dma((N_OUT // K_CUT,)), dma((2,)), dma((7,)), dma((7,)),
            dma((8,)), dma((8,)), dma((4,)),
            dma, dma, dma((3,)), dma((3,)), dma, dma,
            dma((SP // 2,)), dma((SP // 2,)), dma((SP // 2,)), dma((SP // 2,)),
        ],
        compiler_params=pltpu.CompilerParams(
            collective_id=0, has_side_effects=True, vmem_limit_bytes=36 * 1024 * 1024),
        name='decode_step',
    )(*(x if x is freq else pltpu.with_memory_space_constraint(x, pltpu.HBM) for x in (
        hidden, norm_w.reshape(-1, D), b_q.reshape(-1, D), b_k.reshape(1, -1), b_v.reshape(1, -1), freq,
        positions.reshape(1, -1), seq_lens, w_q, w_k, w_v,
        k_cache.reshape(N_ROWS, S_DEV, D), v_cache.reshape(N_ROWS, S_DEV, D), w_o)))


def finish_kernel(ag, kn_rows, vn_rows, hid_ref, y_ref, kn_ref, vn_ref):
    kn_ref[...] = kn_rows[...].astype(BF16)
    vn_ref[...] = vn_rows[...].astype(BF16)
    for zz in range(4):
        for blk in range(12):
            col = slice(zz * N_Z + blk * D, zz * N_Z + (blk + 1) * D)
            for r in range(2):
                rows = slice(PLANE * r, PLANE * (r + 1))
                y_blk = ag[pl.ds(zz * PLANE * AG + r * 12 + blk, PLANE, stride=AG), :]
                y_ref[rows, col] = (hid_ref[rows, col].astype(F32) + y_blk).astype(BF16)


def finish(ag, kn_rows, vn_rows, hidden):
    vmem = pl.BlockSpec(memory_space=pltpu.VMEM)
    return pl.pallas_call(
        finish_kernel,
        out_shape=(jax.ShapeDtypeStruct((N_ROWS, N_OUT), BF16),
                   jax.ShapeDtypeStruct((N_ROWS, D), BF16), jax.ShapeDtypeStruct((N_ROWS, D), BF16)),
        in_specs=[vmem] * 4, out_specs=(vmem,) * 3,
        compiler_params=pltpu.CompilerParams(vmem_limit_bytes=8 * 1024 * 1024),
        name='finish',
    )(ag, kn_rows, vn_rows, hidden)


def solution(mesh):
    def device_step(*operands):
        lane = jnp.arange(D, dtype=jnp.int32)
        inv_freq = ROPE_BASE ** (-2.0 * (lane // 2).astype(jnp.float32) / (D // 2))
        freq = jnp.where(lane < D // 2, inv_freq, 0.0).reshape(1, D)
        y_out, k_new, v_new = finish(*step_call(freq, *operands), operands[0])
        return y_out, k_new.reshape(N_ROWS, 1, D), v_new.reshape(N_ROWS, 1, D)

    col_spec = P(None, 'tp')
    vec_spec = P('tp')
    cache_spec = P('dp', 'sp', 'tp', None)
    group_spec = P('dp', 'tp', None)
    in_specs = (P('dp', None), P(None), col_spec, vec_spec, col_spec, vec_spec, col_spec, vec_spec,
                P('tp', None), cache_spec, cache_spec, P('dp'), P('dp'))
    out_specs = (P('dp', None), group_spec, group_spec)
    return jax.shard_map(device_step, mesh=mesh, in_specs=in_specs, out_specs=out_specs, check_vma=False)
```

```python
import functools
import math

import jax
import jax.numpy as jnp
from jax import lax
from jax.experimental import pallas as pl
from jax.experimental.pallas import tpu as pltpu
from jax.sharding import PartitionSpec as P

RMS_EPS = 1.5625e-7
ROPE_BASE = 10000.0
NEG_BIG = -3.0e38
MESH = pl.DeviceIdType.MESH
F32 = jnp.float32
BF16 = jnp.bfloat16

N_ROWS = 32
S_DEV = 512
D = 128
SP = 64
PLANE = 16
HEADS = 24
SLOT = 32
N_OUT = 6144
K_OUT = 3072
N_CUT = 1024
WO_SLOTS = 5
Q_DEV = 384
K_CUT = 1536


def step_kernel(hid_hbm, nw_hbm, bq_hbm, bk_hbm, bv_hbm, freq_ref, pos_hbm, seq_hbm,
                wq_hbm, wk_hbm, wv_hbm, k_hbm, v_hbm, wo_hbm, y_own, y_other, kn_rows, vn_rows,
                nw_ref, bq_ref, bk_ref, bv_ref, pos_ref, seq_ref, hid_ref, normed, wqbuf, wkvbuf, bq_rows, q_all,
                kbuf, vbuf, wobuf, o_send, o_recv, ag, lhs,
                vecsem, hsem, wqsem, wkvsem, q_send, q_recv,
                ksem, vsem, wsem, rs_send, rs_recv, ag_send, ag_recv, d_send, d_recv):
    c = lax.axis_index('tp')
    s = lax.axis_index('sp')
    z = lax.div(s, PLANE)
    p = lax.rem(s, PLANE)
    y_at = lax.div(p, 4)
    x_at = lax.rem(p, 4)
    qk_scale = (D ** -0.5) * math.log2(math.e)

    label = 4 * lax.rem(z, 2) + 2 * lax.rem(y_at, 2) + lax.rem(x_at, 2)
    hid_copy = pltpu.make_async_copy(hid_hbm, hid_ref, hsem)
    hid_copy.start()
    vec_copies = [pltpu.make_async_copy(src, dst, vecsem.at[j]) for j, (src, dst) in enumerate((
        (pos_hbm, pos_ref), (nw_hbm, nw_ref), (bq_hbm, bq_ref), (bk_hbm, bk_ref), (bv_hbm, bv_ref), (seq_hbm, seq_ref)))]
    for cp in vec_copies:
        cp.start()
    q_cols = pl.ds(pl.multiple_of(label * Q_DEV, D), Q_DEV)
    wq_copies = [pltpu.make_async_copy(
        wq_hbm.at[pl.ds(K_CUT * j, K_CUT), q_cols], wqbuf.at[pl.ds(K_CUT * j, K_CUT)], wqsem.at[j])
        for j in range(N_OUT // K_CUT)]
    for cp in wq_copies:
        cp.start()

    barrier = pltpu.get_barrier_semaphore()

    def greet(d, carry):
        pl.semaphore_signal(barrier, inc=1, device_id={'sp': lax.rem(s + d, SP)}, device_id_type=MESH)
        return carry
    lax.fori_loop(1, SP, greet, 0)
    pl.semaphore_signal(barrier, inc=1, device_id={'tp': 1 - c}, device_id_type=MESH)

    wkv_copies = [pltpu.make_async_copy(wk_hbm, wkvbuf.at[:, pl.ds(0, D)], wkvsem.at[0]),
                  pltpu.make_async_copy(wv_hbm, wkvbuf.at[:, pl.ds(D, D)], wkvsem.at[1])]
    for cp in wkv_copies:
        cp.start()

    own = lax.div(s, 2)
    is_owner = lax.rem(s, 2) == c

    def group_of(g):
        return lax.rem(lax.div(own, 4) + 1 + g, 8)

    def kv_copies(g):
        rows = pl.ds(4 * group_of(g), 4)
        return [pltpu.make_async_copy(k_hbm.at[rows], kbuf.at[rows], ksem.at[g]),
                pltpu.make_async_copy(v_hbm.at[rows], vbuf.at[rows], vsem.at[g])]
    wo_copies = [pltpu.make_async_copy(
        wo_hbm.at[:, pl.ds(N_CUT * j, N_CUT)], wobuf.at[j % WO_SLOTS], wsem.at[j]) for j in range(N_OUT // N_CUT)]

    vec_copies[0].wait()
    row_eye = lax.broadcasted_iota(jnp.int32, (N_ROWS, N_ROWS), 0) == lax.broadcasted_iota(jnp.int32, (N_ROWS, N_ROWS), 1)
    pos_col = jnp.sum(jnp.where(row_eye, pos_ref[...].astype(F32), 0.0), axis=1, keepdims=True)
    angles = pos_col * freq_ref[...]
    is_even = lax.rem(lax.broadcasted_iota(jnp.int32, (N_ROWS, D), 1), 2) == 0
    cos_t = jnp.cos(angles)
    sin_t = jnp.where(is_even, -jnp.sin(angles), jnp.sin(angles))

    def rotate(head):
        other = jnp.where(is_even, pltpu.roll(head, D - 1, 1), pltpu.roll(head, 1, 1))
        return (head * cos_t + other * sin_t).astype(BF16)

    hid_copy.wait()
    for cp in vec_copies[1:]:
        cp.wait()
    x_f32 = hid_ref[...].astype(F32)
    mean_sq = jnp.mean(x_f32 * x_f32, axis=-1, keepdims=True)
    unit = lax.rsqrt(mean_sq + RMS_EPS)
    nw_rows = nw_ref[...].astype(F32)
    for j in range(N_OUT // D):
        cut = slice(j * D, (j + 1) * D)
        normed[:, cut] = (x_f32[:, cut] * unit * nw_rows[j:j + 1, :]).astype(BF16)
    bq_rows[...] = bq_ref[...].astype(F32)

    q_mine = jnp.zeros((N_ROWS, Q_DEV), F32)
    for j, cp in enumerate(wq_copies):
        cp.wait()
        cut = slice(K_CUT * j, K_CUT * (j + 1))
        q_mine = q_mine + jnp.dot(normed[:, cut], wqbuf[cut, :], preferred_element_type=F32)
    for g in range(8):
        for cp in kv_copies(g):
            cp.start()

    def q_rows(lab):
        return pl.multiple_of(lab * (3 * N_ROWS), N_ROWS)
    for t in range(3):
        head = q_mine[:, t * D:(t + 1) * D] + bq_rows[pl.ds(3 * label + t, 1), :]
        q_all[pl.ds(q_rows(label) + t * N_ROWS, N_ROWS), :] = rotate(head.astype(BF16).astype(F32)).astype(F32)

    pl.semaphore_wait(barrier, SP)

    def across(v):
        return lax.rem(v + 4 + (1 - 2 * lax.rem(v, 2)) * (1 - 2 * c), 4)
    q_copies = []
    for mask in range(7, 0, -1):
        zd = across(z) if mask & 4 else z
        yd = across(y_at) if mask & 2 else y_at
        xd = across(x_at) if mask & 1 else x_at
        mine = q_all.at[pl.ds(q_rows(label), 3 * N_ROWS)]
        q_copies.append(pltpu.make_async_remote_copy(
            src_ref=mine, dst_ref=mine, send_sem=q_send.at[mask - 1], recv_sem=q_recv.at[mask - 1],
            device_id={'sp': zd * PLANE + yd * 4 + xd}, device_id_type=MESH))
    for cp in q_copies:
        cp.start()

    for cp in wkv_copies:
        cp.wait()
    kv = jnp.dot(normed[...], wkvbuf[...], preferred_element_type=F32)
    k_new = rotate((kv[:, :D] + bk_ref[...].astype(F32)).astype(BF16).astype(F32))
    v_new = (kv[:, D:] + bv_ref[...].astype(F32)).astype(BF16)
    kn_rows[...] = k_new.astype(F32)
    vn_rows[...] = v_new.astype(F32)
    for cp in q_copies:
        cp.wait_recv()

    for cp in wo_copies[:WO_SLOTS]:
        cp.start()

    eye = (lax.broadcasted_iota(jnp.int32, (HEADS, D), 0) == lax.broadcasted_iota(jnp.int32, (HEADS, D), 1))
    stat_row = lax.broadcasted_iota(jnp.int32, (SLOT - HEADS, D), 0)
    pos = s * S_DEV + lax.broadcasted_iota(jnp.int32, (HEADS, S_DEV), 1)
    mine = pl.ds(pl.multiple_of(s * SLOT, SLOT), SLOT)

    def rs_copy(b):
        return pltpu.make_async_remote_copy(
            src_ref=o_send.at[b], dst_ref=o_recv.at[mine],
            send_sem=rs_send, recv_sem=rs_recv, device_id={'sp': 2 * b + c}, device_id_type=MESH)

    def rows_step(step, carry):
        work = []
        for h in range(2):
            for cp in kv_copies(2 * step + h):
                cp.wait()
            work += [4 * group_of(2 * step + h) + lax.rem(own + 1 + u, 4) for u in range(4)]
        scores = []
        for b in work:
            sc = lax.dot_general(q_all[pl.ds(b, HEADS, stride=N_ROWS), :].astype(BF16), kbuf[b],
                                 (((1,), (1,)), ((), ())), preferred_element_type=F32)
            scores.append(jnp.where(pos < seq_ref[b], sc, NEG_BIG))
        tops = [jnp.max(sc, axis=1, keepdims=True) for sc in scores]
        probs = [jnp.exp2((sc - m) * qk_scale) for sc, m in zip(scores, tops)]
        sums = [jnp.sum(pr, axis=1, keepdims=True) for pr in probs]
        for b, m, l, pr in zip(work, tops, sums, probs):
            o_send[b, :HEADS] = jnp.dot(pr.astype(BF16), vbuf[b], preferred_element_type=F32)
            m_row = jnp.sum(jnp.where(eye, m * qk_scale, 0.0), axis=0, keepdims=True)
            l_row = jnp.sum(jnp.where(eye, l, 0.0), axis=0, keepdims=True)
            o_send[b, HEADS:] = jnp.where(stat_row == 0, m_row, l_row)
        for b in work[:-1]:
            rs_copy(b).start()

        @pl.when(2 * work[-1] + c != s)
        def _():
            rs_copy(work[-1]).start()
        return carry
    lax.fori_loop(0, 4, rows_step, 0)

    def all_in(ref, sem):
        pltpu.make_async_copy(ref, ref, sem).wait()

    def ag_copy(dz, dy, dx):
        dest = lax.rem(z + dz, 4) * PLANE + lax.rem(y_at + dy, 4) * 4 + lax.rem(x_at + dx, 4)
        slot = ag.at[pl.ds(pl.multiple_of(own * HEADS, 8), HEADS)]
        return pltpu.make_async_remote_copy(
            src_ref=slot, dst_ref=slot, send_sem=ag_send, recv_sem=ag_recv,
            device_id={'sp': dest}, device_id_type=MESH)
    far_first = sorted(((dz, dy, dx) for dz in range(4) for dy in range(4) for dx in range(4)),
                       key=lambda d: -sum(min(v, 4 - v) for v in d))[:-1]

    @pl.when(is_owner)
    def _():
        o_recv[mine, :] = o_send[own]
        k_mine = kn_rows[pl.ds(own, 1), :]
        v_mine = vn_rows[pl.ds(own, 1), :]
        s_new = jnp.sum(q_all[pl.ds(own, HEADS, stride=N_ROWS), :] * k_mine, axis=1, keepdims=True) * qk_scale
        all_in(o_recv.at[pl.ds(0, (SP - 1) * SLOT)], rs_recv)
        m_rows = o_recv[pl.ds(HEADS, SP, stride=SLOT), :]
        l_rows = o_recv[pl.ds(HEADS + 1, SP, stride=SLOT), :]
        stats = jnp.transpose(jnp.concatenate([m_rows, l_rows], axis=0))[:HEADS]
        m_cols, l_cols = stats[:, :SP], stats[:, SP:]
        m_top = jnp.maximum(jnp.max(m_cols, axis=1, keepdims=True), s_new)
        w_cols = jnp.exp2(m_cols - m_top)
        w_new = jnp.exp2(s_new - m_top)
        l_all = jnp.sum(w_cols * l_cols, axis=1, keepdims=True) + w_new
        acc = w_new * v_mine
        for j in range(SP):
            acc = acc + w_cols[:, j:j + 1] * o_recv[j * SLOT:j * SLOT + HEADS, :]
        ag[pl.ds(pl.multiple_of(own * HEADS, 8), HEADS), :] = acc / l_all
        for d in far_first:
            ag_copy(*d).start()
        all_in(ag.at[pl.ds(0, (N_ROWS - 1) * HEADS)], ag_recv)

    @pl.when(jnp.logical_not(is_owner))
    def _():
        all_in(ag, ag_recv)

    for h in range(HEADS):
        lhs[:, h * D:(h + 1) * D] = ag[pl.ds(h, N_ROWS, stride=HEADS), :].astype(BF16)

    def d_copy(j):
        return pltpu.make_async_remote_copy(
            src_ref=y_own.at[j], dst_ref=y_other.at[j], send_sem=d_send.at[j], recv_sem=d_recv.at[j],
            device_id={'tp': 1 - c}, device_id_type=MESH)

    for j in range(N_OUT // N_CUT):
        wo_copies[j].wait()
        y_own[j] = jnp.dot(lhs[...], wobuf[j % WO_SLOTS], preferred_element_type=F32)
        d_copy(j).start()
        if j + WO_SLOTS < N_OUT // N_CUT:
            wo_copies[j + WO_SLOTS].start()

    @pl.when(is_owner)
    def _():
        all_in(o_send.at[pl.ds(0, N_ROWS - 1)], rs_send)
        all_in(o_recv.at[pl.ds(0, (SP - 1) * HEADS)], ag_send)

    @pl.when(jnp.logical_not(is_owner))
    def _():
        all_in(o_send, rs_send)
    for cp in q_copies:
        cp.wait_send()
    for j in range(N_OUT // N_CUT):
        d_copy(j).wait()


def step_call(freq, *operands):
    hidden, norm_w, w_q, b_q, w_k, b_k, w_v, b_v, w_o, k_cache, v_cache, positions, seq_lens = operands
    vmem = pl.BlockSpec(memory_space=pltpu.VMEM)
    hbm = pl.BlockSpec(memory_space=pltpu.HBM)
    dma = pltpu.SemaphoreType.DMA
    return pl.pallas_call(
        step_kernel,
        out_shape=(jax.ShapeDtypeStruct((N_OUT // N_CUT, N_ROWS, N_CUT), F32),
                   jax.ShapeDtypeStruct((N_OUT // N_CUT, N_ROWS, N_CUT), F32),
                   jax.ShapeDtypeStruct((N_ROWS, D), F32), jax.ShapeDtypeStruct((N_ROWS, D), F32)),
        in_specs=[hbm, hbm, hbm, hbm, hbm, vmem, hbm, hbm, hbm, hbm, hbm, hbm, hbm, hbm],
        out_specs=(vmem,) * 4,
        scratch_shapes=[
            pltpu.VMEM((N_OUT // D, D), BF16),
            pltpu.VMEM((24, D), BF16),
            pltpu.VMEM((1, D), BF16),
            pltpu.VMEM((1, D), BF16),
            pltpu.VMEM((1, N_ROWS), jnp.int32),
            pltpu.SMEM((N_ROWS,), jnp.int32),
            pltpu.VMEM((N_ROWS, N_OUT), BF16),
            pltpu.VMEM((N_ROWS, N_OUT), BF16),
            pltpu.VMEM((N_OUT, Q_DEV), BF16),
            pltpu.VMEM((N_OUT, 2 * D), BF16),
            pltpu.VMEM((24, D), F32),
            pltpu.VMEM((HEADS * N_ROWS, D), F32),
            pltpu.VMEM((N_ROWS, S_DEV, D), BF16),
            pltpu.VMEM((N_ROWS, S_DEV, D), BF16),
            pltpu.VMEM((WO_SLOTS, K_OUT, N_CUT), BF16),
            pltpu.VMEM((N_ROWS, SLOT, D), F32),
            pltpu.VMEM((SP * SLOT, D), F32),
            pltpu.VMEM((N_ROWS * HEADS, D), F32),
            pltpu.VMEM((N_ROWS, K_OUT), BF16),
            dma((6,)), dma, dma((N_OUT // K_CUT,)), dma((2,)), dma((7,)), dma((7,)),
            dma((8,)), dma((8,)), dma((8,)), dma, dma, dma, dma, dma((N_OUT // N_CUT,)), dma((N_OUT // N_CUT,)),
        ],
        compiler_params=pltpu.CompilerParams(
            collective_id=0, has_side_effects=True, vmem_limit_bytes=52 * 1024 * 1024),
        name='decode_step',
    )(*(x if x is freq else pltpu.with_memory_space_constraint(x, pltpu.HBM) for x in (
        hidden, norm_w.reshape(-1, D), b_q.reshape(-1, D), b_k.reshape(1, -1), b_v.reshape(1, -1), freq,
        positions.reshape(1, -1), seq_lens, w_q, w_k, w_v,
        k_cache.reshape(N_ROWS, S_DEV, D), v_cache.reshape(N_ROWS, S_DEV, D), w_o)))


def finish_kernel(y_own, y_other, kn_rows, vn_rows, hid_ref, y_ref, kn_ref, vn_ref):
    kn_ref[...] = kn_rows[...].astype(BF16)
    vn_ref[...] = vn_rows[...].astype(BF16)
    for j in range(N_OUT // N_CUT):
        cut = slice(j * N_CUT, (j + 1) * N_CUT)
        y_ref[:, cut] = (hid_ref[:, cut].astype(F32) + (y_own[j] + y_other[j])).astype(BF16)


def finish(*operands):
    vmem = pl.BlockSpec(memory_space=pltpu.VMEM)
    return pl.pallas_call(
        finish_kernel,
        out_shape=(jax.ShapeDtypeStruct((N_ROWS, N_OUT), BF16),
                   jax.ShapeDtypeStruct((N_ROWS, D), BF16), jax.ShapeDtypeStruct((N_ROWS, D), BF16)),
        in_specs=[vmem] * 5, out_specs=(vmem,) * 3,
        compiler_params=pltpu.CompilerParams(vmem_limit_bytes=4 * 1024 * 1024),
        name='finish',
    )(*operands)


def solution(mesh):
    def device_step(*operands):
        lane = jnp.arange(D, dtype=jnp.int32)
        inv_freq = ROPE_BASE ** (-2.0 * (lane // 2).astype(jnp.float32) / (D // 2))
        freq = jnp.where(lane < D // 2, inv_freq, 0.0).reshape(1, D)
        y_out, k_new, v_new = finish(*step_call(freq, *operands), operands[0])
        return y_out, k_new.reshape(N_ROWS, 1, D), v_new.reshape(N_ROWS, 1, D)

    col_spec = P(None, 'tp')
    vec_spec = P('tp')
    cache_spec = P('dp', 'sp', 'tp', None)
    group_spec = P('dp', 'tp', None)
    in_specs = (P('dp', None), P(None), col_spec, vec_spec, col_spec, vec_spec, col_spec, vec_spec,
                P('tp', None), cache_spec, cache_spec, P('dp'), P('dp'))
    out_specs = (P('dp', None), group_spec, group_spec)
    return jax.shard_map(device_step, mesh=mesh, in_specs=in_specs, out_specs=out_specs, check_vma=False)
```

```python
import functools
import math

import jax
import jax.numpy as jnp
from jax import lax
from jax.experimental import pallas as pl
from jax.experimental.pallas import tpu as pltpu
from jax.sharding import PartitionSpec as P

RMS_EPS = 1.5625e-7
ROPE_BASE = 10000.0
NEG_BIG = -3.0e38
MESH = pl.DeviceIdType.MESH
F32 = jnp.float32
BF16 = jnp.bfloat16

N_ROWS = 32
S_DEV = 512
D = 128
SP = 64
PLANE = 16
HALF = 12
SLOT = 16
N_OUT = 6144
K_HALF = 1536
N_CUT = 1024
AG = 24
Q_DEV = 384
K_CUT = 1536


def step_kernel(hid_hbm, nw_hbm, bq_hbm, bk_hbm, bv_hbm, freq_ref, pos_hbm, seq_hbm,
                wq_hbm, wk_hbm, wv_hbm, k_hbm, v_hbm, wo_hbm, ag, kn_rows, vn_rows,
                nw_ref, bq_ref, bk_ref, bv_ref, pos_ref, seq_ref, hid_ref, normed, wqbuf, wkvbuf, bq_rows, q_all,
                kbuf, vbuf, wobuf, o_send, o_recv, lhs, part, others,
                vecsem, hsem, wqsem, wkvsem, q_send, q_recv,
                ksem, vsem, wsem, rs_send, rs_recv, x_send, x_recv,
                ag_send, ag_recv, f_send, f_recv):
    c = lax.axis_index('tp')
    s = lax.axis_index('sp')
    z = lax.div(s, PLANE)
    p = lax.rem(s, PLANE)
    y_at = lax.div(p, 4)
    x_at = lax.rem(p, 4)
    qk_scale = (D ** -0.5) * math.log2(math.e)

    label = 4 * lax.rem(z, 2) + 2 * lax.rem(y_at, 2) + lax.rem(x_at, 2)
    hid_copy = pltpu.make_async_copy(hid_hbm, hid_ref, hsem)
    hid_copy.start()
    vec_copies = [pltpu.make_async_copy(src, dst, vecsem.at[j]) for j, (src, dst) in enumerate((
        (pos_hbm, pos_ref), (nw_hbm, nw_ref), (bq_hbm, bq_ref), (bk_hbm, bk_ref), (bv_hbm, bv_ref), (seq_hbm, seq_ref)))]
    for cp in vec_copies:
        cp.start()
    q_cols = pl.ds(pl.multiple_of(label * Q_DEV, D), Q_DEV)
    wq_copies = [pltpu.make_async_copy(
        wq_hbm.at[pl.ds(K_CUT * j, K_CUT), q_cols], wqbuf.at[pl.ds(K_CUT * j, K_CUT)], wqsem.at[j])
        for j in range(N_OUT // K_CUT)]
    for cp in wq_copies:
        cp.start()

    barrier = pltpu.get_barrier_semaphore()

    def greet(d, carry):
        pl.semaphore_signal(barrier, inc=1, device_id={'sp': lax.rem(s + d, SP)}, device_id_type=MESH)
        return carry
    lax.fori_loop(1, SP, greet, 0)
    pl.semaphore_signal(barrier, inc=1, device_id={'tp': 1 - c}, device_id_type=MESH)
    my_half = lax.rem(z, 2)
    near = (z + 1 - 2 * my_half) * PLANE + p
    pl.semaphore_signal(barrier, inc=1, device_id={'sp': near, 'tp': 1 - c}, device_id_type=MESH)

    wkv_copies = [pltpu.make_async_copy(wk_hbm, wkvbuf.at[:, pl.ds(0, D)], wkvsem.at[0]),
                  pltpu.make_async_copy(wv_hbm, wkvbuf.at[:, pl.ds(D, D)], wkvsem.at[1])]
    def kv_copies(step):
        y_to = lax.rem(y_at + 1 + step, 4)
        pairs = []
        for r in range(2):
            rows = pl.ds(PLANE * r + 4 * y_to, 4)
            pairs.append(pltpu.make_async_copy(k_hbm.at[rows], kbuf.at[rows], ksem.at[2 * step + r]))
            pairs.append(pltpu.make_async_copy(v_hbm.at[rows], vbuf.at[rows], vsem.at[2 * step + r]))
        return pairs
    wo_copies = [pltpu.make_async_copy(
        wo_hbm.at[pl.ds(pl.multiple_of(my_half * K_HALF, K_HALF) + 192 * j, 192)], wobuf.at[pl.ds(192 * j, 192)],
        wsem.at[j]) for j in range(8)]

    vec_copies[0].wait()
    row_eye = lax.broadcasted_iota(jnp.int32, (N_ROWS, N_ROWS), 0) == lax.broadcasted_iota(jnp.int32, (N_ROWS, N_ROWS), 1)
    pos_col = jnp.sum(jnp.where(row_eye, pos_ref[...].astype(F32), 0.0), axis=1, keepdims=True)
    angles = pos_col * freq_ref[...]
    is_even = lax.rem(lax.broadcasted_iota(jnp.int32, (N_ROWS, D), 1), 2) == 0
    cos_t = jnp.cos(angles)
    sin_t = jnp.where(is_even, -jnp.sin(angles), jnp.sin(angles))

    def rotate(head):
        other = jnp.where(is_even, pltpu.roll(head, D - 1, 1), pltpu.roll(head, 1, 1))
        return (head * cos_t + other * sin_t).astype(BF16)

    hid_copy.wait()
    for cp in vec_copies[1:]:
        cp.wait()
    x_f32 = hid_ref[...].astype(F32)
    mean_sq = jnp.mean(x_f32 * x_f32, axis=-1, keepdims=True)
    unit = lax.rsqrt(mean_sq + RMS_EPS)
    nw_rows = nw_ref[...].astype(F32)
    for j in range(N_OUT // D):
        cut = slice(j * D, (j + 1) * D)
        normed[:, cut] = (x_f32[:, cut] * unit * nw_rows[j:j + 1, :]).astype(BF16)
    bq_rows[...] = bq_ref[...].astype(F32)

    q_mine = jnp.zeros((N_ROWS, Q_DEV), F32)
    for j, cp in enumerate(wq_copies):
        cp.wait()
        cut = slice(K_CUT * j, K_CUT * (j + 1))
        q_mine = q_mine + jnp.dot(normed[:, cut], wqbuf[cut, :], preferred_element_type=F32)
    for cp in wkv_copies:
        cp.start()
    for step in range(4):
        for cp in kv_copies(step):
            cp.start()
    for cp in wo_copies:
        cp.start()
    for hf in range(2):
        q_all[pl.ds((hf * SLOT + HALF) * N_ROWS, (SLOT - HALF) * N_ROWS), :] = jnp.zeros(((SLOT - HALF) * N_ROWS, D), F32)

    def q_rows(lab):
        first = lax.div(lab, 4) * SLOT + 3 * lax.rem(lab, 4)
        return pl.multiple_of(first * N_ROWS, N_ROWS)
    for t in range(3):
        head = q_mine[:, t * D:(t + 1) * D] + bq_rows[pl.ds(3 * label + t, 1), :]
        q_all[pl.ds(q_rows(label) + t * N_ROWS, N_ROWS), :] = rotate(head.astype(BF16).astype(F32)).astype(F32)

    pl.semaphore_wait(barrier, SP + 1)

    def across(v):
        return lax.rem(v + 4 + (1 - 2 * lax.rem(v, 2)) * (1 - 2 * c), 4)
    q_copies = []
    for mask in range(7, 0, -1):
        zd = across(z) if mask & 4 else z
        yd = across(y_at) if mask & 2 else y_at
        xd = across(x_at) if mask & 1 else x_at
        mine = q_all.at[pl.ds(q_rows(label), 3 * N_ROWS)]
        q_copies.append(pltpu.make_async_remote_copy(
            src_ref=mine, dst_ref=mine, send_sem=q_send.at[mask - 1], recv_sem=q_recv.at[mask - 1],
            device_id={'sp': zd * PLANE + yd * 4 + xd}, device_id_type=MESH))
    for cp in q_copies:
        cp.start()

    for cp in wkv_copies:
        cp.wait()
    kv = jnp.dot(normed[...], wkvbuf[...], preferred_element_type=F32)
    k_new = rotate((kv[:, :D] + bk_ref[...].astype(F32)).astype(BF16).astype(F32))
    v_new = (kv[:, D:] + bv_ref[...].astype(F32)).astype(BF16)
    kn_rows[...] = k_new.astype(F32)
    vn_rows[...] = v_new.astype(F32)
    for cp in q_copies:
        cp.wait_recv()

    lane = lax.broadcasted_iota(jnp.int32, (SLOT, D), 1)
    sub = lax.broadcasted_iota(jnp.int32, (SLOT, D), 0)
    eye = lane == sub
    pos = s * S_DEV + lax.broadcasted_iota(jnp.int32, (2 * SLOT, S_DEV), 1)

    def rs_copy(dest):
        return pltpu.make_async_remote_copy(
            src_ref=o_send.at[dest], dst_ref=o_recv.at[pl.ds(pl.multiple_of(s * SLOT, SLOT), SLOT)],
            send_sem=rs_send, recv_sem=rs_recv, device_id={'sp': dest}, device_id_type=MESH)

    def rows_step(step, carry):
        y_to = lax.rem(y_at + 1 + step, 4)
        for cp in kv_copies(step):
            cp.wait()
        work = []
        for u in range(4):
            for r in range(2):
                chip = 4 * y_to + lax.rem(x_at + 1 + u, 4)
                work.append((u, r, chip, chip + PLANE * r))
        scores = []
        for u, r, chip, b in work:
            sc = lax.dot_general(q_all[pl.ds(b, 2 * SLOT, stride=N_ROWS), :].astype(BF16), kbuf[b],
                                 (((1,), (1,)), ((), ())), preferred_element_type=F32)
            scores.append(jnp.where(pos < seq_ref[b], sc, NEG_BIG))
        tops = [jnp.max(sc, axis=1, keepdims=True) for sc in scores]
        probs = [jnp.exp2((sc - m) * qk_scale) for sc, m in zip(scores, tops)]
        sums = [jnp.sum(pr, axis=1, keepdims=True) for pr in probs]
        for (u, r, chip, b), m, l, pr in zip(work, tops, sums, probs):
            o = jnp.dot(pr.astype(BF16), vbuf[b], preferred_element_type=F32)
            m2 = m * qk_scale
            for hf in range(2):
                part = slice(hf * SLOT, (hf + 1) * SLOT)
                m_row = jnp.sum(jnp.where(eye, m2[part], 0.0), axis=0, keepdims=True)
                l_row = jnp.sum(jnp.where(eye, l[part], 0.0), axis=0, keepdims=True)
                o_send[(2 * r + hf) * PLANE + chip] = jnp.where(
                    sub == HALF, m_row, jnp.where(sub == HALF + 1, l_row, o[part]))
        for u, r, chip, b in work:
            for hf in range(2):
                dest = (2 * r + hf) * PLANE + chip
                if u < 3:
                    rs_copy(dest).start()
                else:
                    @pl.when(dest != s)
                    def _():
                        rs_copy(dest).start()
        return carry
    lax.fori_loop(0, 4, rows_step, 0)
    mine = pl.ds(pl.multiple_of(s * SLOT, SLOT), SLOT)
    o_recv[mine, :] = o_send[s]

    my_row = p + PLANE * lax.div(z, 2)
    q_own = q_all[pl.ds(my_half * SLOT * N_ROWS + my_row, SLOT, stride=N_ROWS), :]
    k_mine = kn_rows[pl.ds(my_row, 1), :]
    v_mine = vn_rows[pl.ds(my_row, 1), :]
    s_new = jnp.sum(q_own * k_mine, axis=1, keepdims=True) * qk_scale

    def all_in(ref, sem):
        pltpu.make_async_copy(ref, ref, sem).wait()

    all_in(o_recv.at[pl.ds(0, (SP - 1) * SLOT)], rs_recv)
    m_rows = o_recv[pl.ds(HALF, SP, stride=SLOT), :]
    l_rows = o_recv[pl.ds(HALF + 1, SP, stride=SLOT), :]
    stats = jnp.transpose(jnp.concatenate([m_rows, l_rows], axis=0))[:SLOT]
    m_cols, l_cols = stats[:, :SP], stats[:, SP:]
    m_top = jnp.maximum(jnp.max(m_cols, axis=1, keepdims=True), s_new)
    w_cols = jnp.exp2(m_cols - m_top)
    w_new = jnp.exp2(s_new - m_top)
    l_all = jnp.sum(w_cols * l_cols, axis=1, keepdims=True) + w_new
    acc = w_new * v_mine
    for j in range(SP):
        acc = acc + w_cols[:, j:j + 1] * o_recv[j * SLOT:(j + 1) * SLOT, :]
    attn = acc / l_all
    lhs[...] = jnp.zeros_like(lhs)
    for j in range(HALF):
        lhs[0:1, j * D:(j + 1) * D] = attn[j:j + 1, :]
    for cp in wo_copies:
        cp.wait()

    lhs_b16 = lhs[...].astype(BF16)
    for n in range(N_OUT // N_CUT):
        piece = jnp.dot(lhs_b16, wobuf[:, n * N_CUT:(n + 1) * N_CUT], preferred_element_type=F32)
        half, first = n // 3, (n % 3) * (N_CUT // D)
        for j in range(N_CUT // D):
            row = first + j
            part[pl.ds(lax.rem(half + my_half, 2) * AG + row, 1), :] = piece[0:1, j * D:(j + 1) * D]
    own_part, other_part = part.at[pl.ds(0, AG)], part.at[pl.ds(AG, AG)]
    x_copies = [
        pltpu.make_async_remote_copy(src_ref=other_part, dst_ref=others.at[0], send_sem=x_send.at[0], recv_sem=x_recv.at[0],
                                     device_id={'sp': near, 'tp': 1 - c}, device_id_type=MESH),
        pltpu.make_async_remote_copy(src_ref=other_part, dst_ref=others.at[1], send_sem=x_send.at[1], recv_sem=x_recv.at[1],
                                     device_id={'sp': near}, device_id_type=MESH),
        pltpu.make_async_remote_copy(src_ref=own_part, dst_ref=others.at[2], send_sem=x_send.at[2], recv_sem=x_recv.at[2],
                                     device_id={'tp': 1 - c}, device_id_type=MESH)]
    for cp in x_copies:
        cp.start()
    for cp in x_copies:
        cp.wait_recv()

    def ag_slot(i):
        return ag.at[pl.ds(pl.multiple_of(i * AG, 8), AG)]
    ag[pl.ds(pl.multiple_of(s * AG, 8), AG), :] = (part[:AG, :] + others[2]) + (others[0] + others[1])

    offsets = sorted(((dz, dy, j) for dz in range(4) for dy in range(4) for j in range(2)),
                     key=lambda d: min(d[0], 4 - d[0]) + min(d[1], 4 - d[1]) + 1.5 * d[2])

    def chip_at(dz, dy, dx):
        return lax.rem(z + dz, 4) * PLANE + lax.rem(y_at + dy, 4) * 4 + lax.rem(x_at + dx, 4)

    def ag_copy(n):
        dz, dy, j = offsets[n]
        return pltpu.make_async_remote_copy(
            src_ref=ag_slot(s), dst_ref=ag_slot(s), send_sem=ag_send, recv_sem=ag_recv.at[n],
            device_id={'sp': chip_at(dz, dy, 2 * j + c)}, device_id_type=MESH)

    def forward(n):
        dz, dy, j = offsets[n]
        slot = ag_slot(chip_at(4 - dz, 4 - dy, 4 - 2 * j - c))
        return slot, pltpu.make_async_remote_copy(
            src_ref=slot, dst_ref=slot, send_sem=f_send, recv_sem=f_recv, device_id={'tp': 1 - c}, device_id_type=MESH)

    def relay(n):
        slot, cp = forward(n)
        pltpu.make_async_copy(slot, slot, ag_recv.at[n]).wait()
        cp.start()

    for n in range(SP // 2 - 1, 0, -1):
        ag_copy(n).start()

    @pl.when(c == 1)
    def _():
        ag_copy(0).start()
        relay(0)
    for n in range(1, SP // 2):
        relay(n)

    few, many = ag.at[pl.ds(0, (SP // 2 - 1) * AG)], ag.at[pl.ds(0, SP // 2 * AG)]

    @pl.when(c == 0)
    def _():
        all_in(many, f_recv)
        all_in(few, f_send)
        all_in(few, ag_send)

    @pl.when(c == 1)
    def _():
        all_in(few, f_recv)
        all_in(many, f_send)
        all_in(many, ag_send)
    all_in(o_send.at[pl.ds(0, SP - 1)], rs_send)
    for cp in q_copies + x_copies:
        cp.wait_send()


def step_call(freq, *operands):
    hidden, norm_w, w_q, b_q, w_k, b_k, w_v, b_v, w_o, k_cache, v_cache, positions, seq_lens = operands
    vmem = pl.BlockSpec(memory_space=pltpu.VMEM)
    hbm = pl.BlockSpec(memory_space=pltpu.HBM)
    dma = pltpu.SemaphoreType.DMA
    return pl.pallas_call(
        step_kernel,
        out_shape=(jax.ShapeDtypeStruct((SP * AG, D), F32),
                   jax.ShapeDtypeStruct((N_ROWS, D), F32), jax.ShapeDtypeStruct((N_ROWS, D), F32)),
        in_specs=[hbm, hbm, hbm, hbm, hbm, vmem, hbm, hbm, hbm, hbm, hbm, hbm, hbm, hbm],
        out_specs=(vmem, vmem, vmem),
        scratch_shapes=[
            pltpu.VMEM((N_OUT // D, D), BF16),
            pltpu.VMEM((24, D), BF16),
            pltpu.VMEM((1, D), BF16),
            pltpu.VMEM((1, D), BF16),
            pltpu.VMEM((1, N_ROWS), jnp.int32),
            pltpu.SMEM((N_ROWS,), jnp.int32),
            pltpu.VMEM((N_ROWS, N_OUT), BF16),
            pltpu.VMEM((N_ROWS, N_OUT), BF16),
            pltpu.VMEM((N_OUT, Q_DEV), BF16),
            pltpu.VMEM((N_OUT, 2 * D), BF16),
            pltpu.VMEM((24, D), F32),
            pltpu.VMEM((2 * SLOT * N_ROWS, D), F32),
            pltpu.VMEM((N_ROWS, S_DEV, D), BF16),
            pltpu.VMEM((N_ROWS, S_DEV, D), BF16),
            pltpu.VMEM((K_HALF, N_OUT), BF16),
            pltpu.VMEM((2 * N_ROWS, SLOT, D), F32),
            pltpu.VMEM((SP * SLOT, D), F32),
            pltpu.VMEM((8, K_HALF), F32),
            pltpu.VMEM((2 * AG, D), F32),
            pltpu.VMEM((3, AG, D), F32),
            dma((6,)), dma, dma((N_OUT // K_CUT,)), dma((2,)), dma((7,)), dma((7,)),
            dma((8,)), dma((8,)), dma((8,)), dma, dma, dma((3,)), dma((3,)),
            dma, dma((SP // 2,)), dma, dma,
        ],
        compiler_params=pltpu.CompilerParams(
            collective_id=0, has_side_effects=True, vmem_limit_bytes=44 * 1024 * 1024),
        name='decode_step',
    )(*(x if x is freq else pltpu.with_memory_space_constraint(x, pltpu.HBM) for x in (
        hidden, norm_w.reshape(-1, D), b_q.reshape(-1, D), b_k.reshape(1, -1), b_v.reshape(1, -1), freq,
        positions.reshape(1, -1), seq_lens, w_q, w_k, w_v,
        k_cache.reshape(N_ROWS, S_DEV, D), v_cache.reshape(N_ROWS, S_DEV, D), w_o)))


def finish_kernel(ag, kn_rows, vn_rows, hid_ref, y_ref, kn_ref, vn_ref):
    kn_ref[...] = kn_rows[...].astype(BF16)
    vn_ref[...] = vn_rows[...].astype(BF16)
    for zz in range(4):
        r, hf = zz // 2, zz % 2
        rows = slice(PLANE * r, PLANE * (r + 1))
        for blk in range(AG):
            col = slice(hf * (N_OUT // 2) + blk * D, hf * (N_OUT // 2) + (blk + 1) * D)
            y_blk = ag[pl.ds(zz * PLANE * AG + blk, PLANE, stride=AG), :]
            y_ref[rows, col] = (hid_ref[rows, col].astype(F32) + y_blk).astype(BF16)


def finish(ag, kn_rows, vn_rows, hidden):
    vmem = pl.BlockSpec(memory_space=pltpu.VMEM)
    return pl.pallas_call(
        finish_kernel,
        out_shape=(jax.ShapeDtypeStruct((N_ROWS, N_OUT), BF16),
                   jax.ShapeDtypeStruct((N_ROWS, D), BF16), jax.ShapeDtypeStruct((N_ROWS, D), BF16)),
        in_specs=[vmem] * 4, out_specs=(vmem,) * 3,
        compiler_params=pltpu.CompilerParams(vmem_limit_bytes=8 * 1024 * 1024),
        name='finish',
    )(ag, kn_rows, vn_rows, hidden)


def solution(mesh):
    def device_step(*operands):
        lane = jnp.arange(D, dtype=jnp.int32)
        inv_freq = ROPE_BASE ** (-2.0 * (lane // 2).astype(jnp.float32) / (D // 2))
        freq = jnp.where(lane < D // 2, inv_freq, 0.0).reshape(1, D)
        y_out, k_new, v_new = finish(*step_call(freq, *operands), operands[0])
        return y_out, k_new.reshape(N_ROWS, 1, D), v_new.reshape(N_ROWS, 1, D)

    col_spec = P(None, 'tp')
    vec_spec = P('tp')
    cache_spec = P('dp', 'sp', 'tp', None)
    group_spec = P('dp', 'tp', None)
    in_specs = (P('dp', None), P(None), col_spec, vec_spec, col_spec, vec_spec, col_spec, vec_spec,
                P('tp', None), cache_spec, cache_spec, P('dp'), P('dp'))
    out_specs = (P('dp', None), group_spec, group_spec)
    return jax.shard_map(device_step, mesh=mesh, in_specs=in_specs, out_specs=out_specs, check_vma=False)
```

```python
import functools
import math

import jax
import jax.numpy as jnp
from jax import lax
from jax.experimental import pallas as pl
from jax.experimental.pallas import tpu as pltpu
from jax.sharding import PartitionSpec as P

RMS_EPS = 1.5625e-7
ROPE_BASE = 10000.0
NEG_BIG = -3.0e38
MESH = pl.DeviceIdType.MESH
F32 = jnp.float32
BF16 = jnp.bfloat16

N_ROWS = 32
S_DEV = 512
D = 128
SP = 64
PLANE = 16
HALF = 12
SLOT = 16
N_OUT = 6144
K_HALF = 1536
N_CUT = 1024
AG = 24
Q_DEV = 384
K_CUT = 1536


def step_kernel(hid_hbm, nw_hbm, bq_hbm, bk_hbm, bv_hbm, freq_ref, pos_hbm, seq_hbm,
                wq_hbm, wk_hbm, wv_hbm, k_hbm, v_hbm, wo_hbm, ag, kn_rows, vn_rows,
                nw_ref, bq_ref, bk_ref, bv_ref, pos_ref, seq_ref, hid_ref, normed, wqbuf, wkvbuf, bq_rows, q_all,
                kbuf, vbuf, wobuf, o_send, o_recv, lhs, part, others,
                vecsem, hsem, wqsem, wkvsem, q_send, q_recv,
                ksem, vsem, wsem, rs_send, rs_recv, x_send, x_recv,
                ag_send, ag_recv, f_send, f_recv):
    c = lax.axis_index('tp')
    s = lax.axis_index('sp')
    z = lax.div(s, PLANE)
    p = lax.rem(s, PLANE)
    y_at = lax.div(p, 4)
    x_at = lax.rem(p, 4)
    qk_scale = (D ** -0.5) * math.log2(math.e)

    label = 4 * lax.rem(z, 2) + 2 * lax.rem(y_at, 2) + lax.rem(x_at, 2)
    hid_copy = pltpu.make_async_copy(hid_hbm, hid_ref, hsem)
    hid_copy.start()
    vec_copies = [pltpu.make_async_copy(src, dst, vecsem.at[j]) for j, (src, dst) in enumerate((
        (pos_hbm, pos_ref), (nw_hbm, nw_ref), (bq_hbm, bq_ref), (bk_hbm, bk_ref), (bv_hbm, bv_ref), (seq_hbm, seq_ref)))]
    for cp in vec_copies:
        cp.start()
    q_cols = pl.ds(pl.multiple_of(label * Q_DEV, D), Q_DEV)
    wq_copies = [pltpu.make_async_copy(
        wq_hbm.at[pl.ds(K_CUT * j, K_CUT), q_cols], wqbuf.at[pl.ds(K_CUT * j, K_CUT)], wqsem.at[j])
        for j in range(N_OUT // K_CUT)]
    for cp in wq_copies:
        cp.start()

    barrier = pltpu.get_barrier_semaphore()

    def greet(d, carry):
        pl.semaphore_signal(barrier, inc=1, device_id={'sp': lax.rem(s + d, SP)}, device_id_type=MESH)
        return carry
    lax.fori_loop(1, SP, greet, 0)
    pl.semaphore_signal(barrier, inc=1, device_id={'tp': 1 - c}, device_id_type=MESH)
    my_half = lax.rem(z, 2)
    near = (z + 1 - 2 * my_half) * PLANE + p
    pl.semaphore_signal(barrier, inc=1, device_id={'sp': near, 'tp': 1 - c}, device_id_type=MESH)

    wkv_copies = [pltpu.make_async_copy(wk_hbm, wkvbuf.at[:, pl.ds(0, D)], wkvsem.at[0]),
                  pltpu.make_async_copy(wv_hbm, wkvbuf.at[:, pl.ds(D, D)], wkvsem.at[1])]
    def kv_copies(step):
        y_to = lax.rem(y_at + 1 + step, 4)
        pairs = []
        for r in range(2):
            rows = pl.ds(PLANE * r + 4 * y_to, 4)
            pairs.append(pltpu.make_async_copy(k_hbm.at[rows], kbuf.at[rows], ksem.at[2 * step + r]))
            pairs.append(pltpu.make_async_copy(v_hbm.at[rows], vbuf.at[rows], vsem.at[2 * step + r]))
        return pairs
    wo_copies = [pltpu.make_async_copy(
        wo_hbm.at[pl.ds(pl.multiple_of(my_half * K_HALF, K_HALF) + 192 * j, 192)], wobuf.at[pl.ds(192 * j, 192)],
        wsem.at[j]) for j in range(8)]

    vec_copies[0].wait()
    row_eye = lax.broadcasted_iota(jnp.int32, (N_ROWS, N_ROWS), 0) == lax.broadcasted_iota(jnp.int32, (N_ROWS, N_ROWS), 1)
    pos_col = jnp.sum(jnp.where(row_eye, pos_ref[...].astype(F32), 0.0), axis=1, keepdims=True)
    angles = pos_col * freq_ref[...]
    is_even = lax.rem(lax.broadcasted_iota(jnp.int32, (N_ROWS, D), 1), 2) == 0
    cos_t = jnp.cos(angles)
    sin_t = jnp.where(is_even, -jnp.sin(angles), jnp.sin(angles))

    def rotate(head):
        other = jnp.where(is_even, pltpu.roll(head, D - 1, 1), pltpu.roll(head, 1, 1))
        return (head * cos_t + other * sin_t).astype(BF16)

    hid_copy.wait()
    for cp in vec_copies[1:]:
        cp.wait()
    x_f32 = hid_ref[...].astype(F32)
    mean_sq = jnp.mean(x_f32 * x_f32, axis=-1, keepdims=True)
    unit = lax.rsqrt(mean_sq + RMS_EPS)
    nw_rows = nw_ref[...].astype(F32)
    for j in range(N_OUT // D):
        cut = slice(j * D, (j + 1) * D)
        normed[:, cut] = (x_f32[:, cut] * unit * nw_rows[j:j + 1, :]).astype(BF16)
    bq_rows[...] = bq_ref[...].astype(F32)

    q_mine = jnp.zeros((N_ROWS, Q_DEV), F32)
    for j, cp in enumerate(wq_copies):
        cp.wait()
        cut = slice(K_CUT * j, K_CUT * (j + 1))
        q_mine = q_mine + jnp.dot(normed[:, cut], wqbuf[cut, :], preferred_element_type=F32)
    for cp in wkv_copies:
        cp.start()
    for step in range(4):
        for cp in kv_copies(step):
            cp.start()
    for hf in range(2):
        q_all[pl.ds((hf * SLOT + HALF) * N_ROWS, (SLOT - HALF) * N_ROWS), :] = jnp.zeros(((SLOT - HALF) * N_ROWS, D), F32)

    def q_rows(lab):
        first = lax.div(lab, 4) * SLOT + 3 * lax.rem(lab, 4)
        return pl.multiple_of(first * N_ROWS, N_ROWS)
    for t in range(3):
        head = q_mine[:, t * D:(t + 1) * D] + bq_rows[pl.ds(3 * label + t, 1), :]
        q_all[pl.ds(q_rows(label) + t * N_ROWS, N_ROWS), :] = rotate(head.astype(BF16).astype(F32)).astype(F32)

    pl.semaphore_wait(barrier, SP + 1)

    def across(v):
        return lax.rem(v + 4 + (1 - 2 * lax.rem(v, 2)) * (1 - 2 * c), 4)
    q_copies = []
    for mask in range(7, 0, -1):
        zd = across(z) if mask & 4 else z
        yd = across(y_at) if mask & 2 else y_at
        xd = across(x_at) if mask & 1 else x_at
        mine = q_all.at[pl.ds(q_rows(label), 3 * N_ROWS)]
        q_copies.append(pltpu.make_async_remote_copy(
            src_ref=mine, dst_ref=mine, send_sem=q_send.at[mask - 1], recv_sem=q_recv.at[mask - 1],
            device_id={'sp': zd * PLANE + yd * 4 + xd}, device_id_type=MESH))
    for cp in q_copies:
        cp.start()

    for cp in wkv_copies:
        cp.wait()
    kv = jnp.dot(normed[...], wkvbuf[...], preferred_element_type=F32)
    k_new = rotate((kv[:, :D] + bk_ref[...].astype(F32)).astype(BF16).astype(F32))
    v_new = (kv[:, D:] + bv_ref[...].astype(F32)).astype(BF16)
    kn_rows[...] = k_new.astype(F32)
    vn_rows[...] = v_new.astype(F32)
    for cp in q_copies:
        cp.wait_recv()

    lane = lax.broadcasted_iota(jnp.int32, (SLOT, D), 1)
    sub = lax.broadcasted_iota(jnp.int32, (SLOT, D), 0)
    eye = lane == sub
    pos = s * S_DEV + lax.broadcasted_iota(jnp.int32, (2 * SLOT, S_DEV), 1)

    def rs_copy(dest):
        return pltpu.make_async_remote_copy(
            src_ref=o_send.at[dest], dst_ref=o_recv.at[pl.ds(pl.multiple_of(s * SLOT, SLOT), SLOT)],
            send_sem=rs_send, recv_sem=rs_recv, device_id={'sp': dest}, device_id_type=MESH)

    def rows_step(step, carry):
        y_to = lax.rem(y_at + 1 + step, 4)
        for cp in kv_copies(step):
            cp.wait()
        work = []
        for u in range(4):
            for r in range(2):
                chip = 4 * y_to + lax.rem(x_at + 1 + u, 4)
                work.append((u, r, chip, chip + PLANE * r))
        scores = []
        for u, r, chip, b in work:
            sc = lax.dot_general(q_all[pl.ds(b, 2 * SLOT, stride=N_ROWS), :].astype(BF16), kbuf[b],
                                 (((1,), (1,)), ((), ())), preferred_element_type=F32)
            scores.append(jnp.where(pos < seq_ref[b], sc, NEG_BIG))
        tops = [jnp.max(sc, axis=1, keepdims=True) for sc in scores]
        probs = [jnp.exp2((sc - m) * qk_scale) for sc, m in zip(scores, tops)]
        sums = [jnp.sum(pr, axis=1, keepdims=True) for pr in probs]
        for (u, r, chip, b), m, l, pr in zip(work, tops, sums, probs):
            o = jnp.dot(pr.astype(BF16), vbuf[b], preferred_element_type=F32)
            m2 = m * qk_scale
            for hf in range(2):
                part = slice(hf * SLOT, (hf + 1) * SLOT)
                m_row = jnp.sum(jnp.where(eye, m2[part], 0.0), axis=0, keepdims=True)
                l_row = jnp.sum(jnp.where(eye, l[part], 0.0), axis=0, keepdims=True)
                o_send[(2 * r + hf) * PLANE + chip] = jnp.where(
                    sub == HALF, m_row, jnp.where(sub == HALF + 1, l_row, o[part]))
        for u, r, chip, b in work:
            for hf in range(2):
                dest = (2 * r + hf) * PLANE + chip
                if u < 3:
                    rs_copy(dest).start()
                else:
                    @pl.when(dest != s)
                    def _():
                        rs_copy(dest).start()
        return carry
    lax.fori_loop(0, 4, rows_step, 0)
    for cp in wo_copies:
        cp.start()
    mine = pl.ds(pl.multiple_of(s * SLOT, SLOT), SLOT)
    o_recv[mine, :] = o_send[s]

    my_row = p + PLANE * lax.div(z, 2)
    q_own = q_all[pl.ds(my_half * SLOT * N_ROWS + my_row, SLOT, stride=N_ROWS), :]
    k_mine = kn_rows[pl.ds(my_row, 1), :]
    v_mine = vn_rows[pl.ds(my_row, 1), :]
    s_new = jnp.sum(q_own * k_mine, axis=1, keepdims=True) * qk_scale

    def all_in(ref, sem):
        pltpu.make_async_copy(ref, ref, sem).wait()

    all_in(o_recv.at[pl.ds(0, (SP - 1) * SLOT)], rs_recv)
    m_rows = o_recv[pl.ds(HALF, SP, stride=SLOT), :]
    l_rows = o_recv[pl.ds(HALF + 1, SP, stride=SLOT), :]
    stats = jnp.transpose(jnp.concatenate([m_rows, l_rows], axis=0))[:SLOT]
    m_cols, l_cols = stats[:, :SP], stats[:, SP:]
    m_top = jnp.maximum(jnp.max(m_cols, axis=1, keepdims=True), s_new)
    w_cols = jnp.exp2(m_cols - m_top)
    w_new = jnp.exp2(s_new - m_top)
    l_all = jnp.sum(w_cols * l_cols, axis=1, keepdims=True) + w_new
    acc = w_new * v_mine
    for j in range(SP):
        acc = acc + w_cols[:, j:j + 1] * o_recv[j * SLOT:(j + 1) * SLOT, :]
    attn = acc / l_all
    lhs[...] = jnp.zeros_like(lhs)
    for j in range(HALF):
        lhs[0:1, j * D:(j + 1) * D] = attn[j:j + 1, :]
    for cp in wo_copies:
        cp.wait()

    lhs_b16 = lhs[...].astype(BF16)
    for n in range(N_OUT // N_CUT):
        piece = jnp.dot(lhs_b16, wobuf[:, n * N_CUT:(n + 1) * N_CUT], preferred_element_type=F32)
        half, first = n // 3, (n % 3) * (N_CUT // D)
        for j in range(N_CUT // D):
            row = first + j
            part[pl.ds(lax.rem(half + my_half, 2) * AG + row, 1), :] = piece[0:1, j * D:(j + 1) * D]
    own_part, other_part = part.at[pl.ds(0, AG)], part.at[pl.ds(AG, AG)]
    x_copies = [
        pltpu.make_async_remote_copy(src_ref=other_part, dst_ref=others.at[0], send_sem=x_send.at[0], recv_sem=x_recv.at[0],
                                     device_id={'sp': near, 'tp': 1 - c}, device_id_type=MESH),
        pltpu.make_async_remote_copy(src_ref=other_part, dst_ref=others.at[1], send_sem=x_send.at[1], recv_sem=x_recv.at[1],
                                     device_id={'sp': near}, device_id_type=MESH),
        pltpu.make_async_remote_copy(src_ref=own_part, dst_ref=others.at[2], send_sem=x_send.at[2], recv_sem=x_recv.at[2],
                                     device_id={'tp': 1 - c}, device_id_type=MESH)]
    for cp in x_copies:
        cp.start()
    for cp in x_copies:
        cp.wait_recv()

    def ag_slot(i):
        return ag.at[pl.ds(pl.multiple_of(i * AG, 8), AG)]
    ag[pl.ds(pl.multiple_of(s * AG, 8), AG), :] = (part[:AG, :] + others[2]) + (others[0] + others[1])

    offsets = sorted(((dz, dy, j) for dz in range(4) for dy in range(4) for j in range(2)),
                     key=lambda d: min(d[0], 4 - d[0]) + min(d[1], 4 - d[1]) + 1.5 * d[2])

    def chip_at(dz, dy, dx):
        return lax.rem(z + dz, 4) * PLANE + lax.rem(y_at + dy, 4) * 4 + lax.rem(x_at + dx, 4)

    def ag_copy(n):
        dz, dy, j = offsets[n]
        return pltpu.make_async_remote_copy(
            src_ref=ag_slot(s), dst_ref=ag_slot(s), send_sem=ag_send, recv_sem=ag_recv.at[n],
            device_id={'sp': chip_at(dz, dy, 2 * j + c)}, device_id_type=MESH)

    def forward(n):
        dz, dy, j = offsets[n]
        slot = ag_slot(chip_at(4 - dz, 4 - dy, 4 - 2 * j - c))
        return slot, pltpu.make_async_remote_copy(
            src_ref=slot, dst_ref=slot, send_sem=f_send, recv_sem=f_recv, device_id={'tp': 1 - c}, device_id_type=MESH)

    def relay(n):
        slot, cp = forward(n)
        pltpu.make_async_copy(slot, slot, ag_recv.at[n]).wait()
        cp.start()

    for n in range(SP // 2 - 1, 0, -1):
        ag_copy(n).start()

    @pl.when(c == 1)
    def _():
        ag_copy(0).start()
        relay(0)
    for n in range(1, SP // 2):
        relay(n)

    few, many = ag.at[pl.ds(0, (SP // 2 - 1) * AG)], ag.at[pl.ds(0, SP // 2 * AG)]

    @pl.when(c == 0)
    def _():
        all_in(many, f_recv)
        all_in(few, f_send)
        all_in(few, ag_send)

    @pl.when(c == 1)
    def _():
        all_in(few, f_recv)
        all_in(many, f_send)
        all_in(many, ag_send)
    all_in(o_send.at[pl.ds(0, SP - 1)], rs_send)
    for cp in q_copies + x_copies:
        cp.wait_send()


def step_call(freq, *operands):
    hidden, norm_w, w_q, b_q, w_k, b_k, w_v, b_v, w_o, k_cache, v_cache, positions, seq_lens = operands
    vmem = pl.BlockSpec(memory_space=pltpu.VMEM)
    hbm = pl.BlockSpec(memory_space=pltpu.HBM)
    dma = pltpu.SemaphoreType.DMA
    return pl.pallas_call(
        step_kernel,
        out_shape=(jax.ShapeDtypeStruct((SP * AG, D), F32),
                   jax.ShapeDtypeStruct((N_ROWS, D), F32), jax.ShapeDtypeStruct((N_ROWS, D), F32)),
        in_specs=[hbm, hbm, hbm, hbm, hbm, vmem, hbm, hbm, hbm, hbm, hbm, hbm, hbm, hbm],
        out_specs=(vmem, vmem, vmem),
        scratch_shapes=[
            pltpu.VMEM((N_OUT // D, D), BF16),
            pltpu.VMEM((24, D), BF16),
            pltpu.VMEM((1, D), BF16),
            pltpu.VMEM((1, D), BF16),
            pltpu.VMEM((1, N_ROWS), jnp.int32),
            pltpu.SMEM((N_ROWS,), jnp.int32),
            pltpu.VMEM((N_ROWS, N_OUT), BF16),
            pltpu.VMEM((N_ROWS, N_OUT), BF16),
            pltpu.VMEM((N_OUT, Q_DEV), BF16),
            pltpu.VMEM((N_OUT, 2 * D), BF16),
            pltpu.VMEM((24, D), F32),
            pltpu.VMEM((2 * SLOT * N_ROWS, D), F32),
            pltpu.VMEM((N_ROWS, S_DEV, D), BF16),
            pltpu.VMEM((N_ROWS, S_DEV, D), BF16),
            pltpu.VMEM((K_HALF, N_OUT), BF16),
            pltpu.VMEM((2 * N_ROWS, SLOT, D), F32),
            pltpu.VMEM((SP * SLOT, D), F32),
            pltpu.VMEM((8, K_HALF), F32),
            pltpu.VMEM((2 * AG, D), F32),
            pltpu.VMEM((3, AG, D), F32),
            dma((6,)), dma, dma((N_OUT // K_CUT,)), dma((2,)), dma((7,)), dma((7,)),
            dma((8,)), dma((8,)), dma((8,)), dma, dma, dma((3,)), dma((3,)),
            dma, dma((SP // 2,)), dma, dma,
        ],
        compiler_params=pltpu.CompilerParams(
            collective_id=0, has_side_effects=True, vmem_limit_bytes=44 * 1024 * 1024),
        name='decode_step',
    )(*(x if x is freq else pltpu.with_memory_space_constraint(x, pltpu.HBM) for x in (
        hidden, norm_w.reshape(-1, D), b_q.reshape(-1, D), b_k.reshape(1, -1), b_v.reshape(1, -1), freq,
        positions.reshape(1, -1), seq_lens, w_q, w_k, w_v,
        k_cache.reshape(N_ROWS, S_DEV, D), v_cache.reshape(N_ROWS, S_DEV, D), w_o)))


def finish_kernel(ag, kn_rows, vn_rows, hid_ref, y_ref, kn_ref, vn_ref):
    kn_ref[...] = kn_rows[...].astype(BF16)
    vn_ref[...] = vn_rows[...].astype(BF16)
    for zz in range(4):
        r, hf = zz // 2, zz % 2
        rows = slice(PLANE * r, PLANE * (r + 1))
        for blk in range(AG):
            col = slice(hf * (N_OUT // 2) + blk * D, hf * (N_OUT // 2) + (blk + 1) * D)
            y_blk = ag[pl.ds(zz * PLANE * AG + blk, PLANE, stride=AG), :]
            y_ref[rows, col] = (hid_ref[rows, col].astype(F32) + y_blk).astype(BF16)


def finish(ag, kn_rows, vn_rows, hidden):
    vmem = pl.BlockSpec(memory_space=pltpu.VMEM)
    return pl.pallas_call(
        finish_kernel,
        out_shape=(jax.ShapeDtypeStruct((N_ROWS, N_OUT), BF16),
                   jax.ShapeDtypeStruct((N_ROWS, D), BF16), jax.ShapeDtypeStruct((N_ROWS, D), BF16)),
        in_specs=[vmem] * 4, out_specs=(vmem,) * 3,
        compiler_params=pltpu.CompilerParams(vmem_limit_bytes=8 * 1024 * 1024),
        name='finish',
    )(ag, kn_rows, vn_rows, hidden)


def solution(mesh):
    def device_step(*operands):
        lane = jnp.arange(D, dtype=jnp.int32)
        inv_freq = ROPE_BASE ** (-2.0 * (lane // 2).astype(jnp.float32) / (D // 2))
        freq = jnp.where(lane < D // 2, inv_freq, 0.0).reshape(1, D)
        y_out, k_new, v_new = finish(*step_call(freq, *operands), operands[0])
        return y_out, k_new.reshape(N_ROWS, 1, D), v_new.reshape(N_ROWS, 1, D)

    col_spec = P(None, 'tp')
    vec_spec = P('tp')
    cache_spec = P('dp', 'sp', 'tp', None)
    group_spec = P('dp', 'tp', None)
    in_specs = (P('dp', None), P(None), col_spec, vec_spec, col_spec, vec_spec, col_spec, vec_spec,
                P('tp', None), cache_spec, cache_spec, P('dp'), P('dp'))
    out_specs = (P('dp', None), group_spec, group_spec)
    return jax.shard_map(device_step, mesh=mesh, in_specs=in_specs, out_specs=out_specs, check_vma=False)
```

```python
import functools
import math

import jax
import jax.numpy as jnp
from jax import lax
from jax.experimental import pallas as pl
from jax.experimental.pallas import tpu as pltpu
from jax.sharding import PartitionSpec as P

RMS_EPS = 1.5625e-7
ROPE_BASE = 10000.0
NEG_BIG = -3.0e38
MESH = pl.DeviceIdType.MESH
F32 = jnp.float32
BF16 = jnp.bfloat16

N_ROWS = 32
S_DEV = 512
D = 128
SP = 64
PLANE = 16
HALF = 12
SLOT = 16
N_OUT = 6144
K_HALF = 1536
N_CUT = 1024
AG = 24
Q_DEV = 384
K_CUT = 1536


def step_kernel(hid_hbm, nw_hbm, bq_hbm, bk_hbm, bv_hbm, freq_ref, pos_hbm, seq_hbm,
                wq_hbm, wk_hbm, wv_hbm, k_hbm, v_hbm, wo_hbm, ag, kn_rows, vn_rows,
                nw_ref, bq_ref, bk_ref, bv_ref, pos_ref, seq_ref, hid_ref, normed, wqbuf, wkvbuf, bq_rows, q_all,
                kbuf, vbuf, wobuf, o_send, o_recv, lhs, part, others,
                vecsem, hsem, wqsem, wkvsem, q_send, q_recv,
                ksem, vsem, wsem, rs_send, rs_recv, x_send, x_recv,
                ag_send, ag_recv, f_send, f_recv):
    c = lax.axis_index('tp')
    s = lax.axis_index('sp')
    z = lax.div(s, PLANE)
    p = lax.rem(s, PLANE)
    y_at = lax.div(p, 4)
    x_at = lax.rem(p, 4)
    qk_scale = (D ** -0.5) * math.log2(math.e)

    label = 4 * lax.rem(z, 2) + 2 * lax.rem(y_at, 2) + lax.rem(x_at, 2)
    hid_copy = pltpu.make_async_copy(hid_hbm, hid_ref, hsem)
    hid_copy.start()
    vec_copies = [pltpu.make_async_copy(src, dst, vecsem.at[j]) for j, (src, dst) in enumerate((
        (pos_hbm, pos_ref), (nw_hbm, nw_ref), (bq_hbm, bq_ref), (bk_hbm, bk_ref), (bv_hbm, bv_ref), (seq_hbm, seq_ref)))]
    for cp in vec_copies:
        cp.start()
    q_cols = pl.ds(pl.multiple_of(label * Q_DEV, D), Q_DEV)
    wq_copies = [pltpu.make_async_copy(
        wq_hbm.at[pl.ds(K_CUT * j, K_CUT), q_cols], wqbuf.at[pl.ds(K_CUT * j, K_CUT)], wqsem.at[j])
        for j in range(N_OUT // K_CUT)]
    for cp in wq_copies:
        cp.start()

    barrier = pltpu.get_barrier_semaphore()

    def greet(d, carry):
        pl.semaphore_signal(barrier, inc=1, device_id={'sp': lax.rem(s + d, SP)}, device_id_type=MESH)
        return carry
    lax.fori_loop(1, SP, greet, 0)
    pl.semaphore_signal(barrier, inc=1, device_id={'tp': 1 - c}, device_id_type=MESH)
    my_half = lax.rem(z, 2)
    near = (z + 1 - 2 * my_half) * PLANE + p
    pl.semaphore_signal(barrier, inc=1, device_id={'sp': near, 'tp': 1 - c}, device_id_type=MESH)

    wkv_copies = [pltpu.make_async_copy(wk_hbm, wkvbuf.at[:, pl.ds(0, D)], wkvsem.at[0]),
                  pltpu.make_async_copy(wv_hbm, wkvbuf.at[:, pl.ds(D, D)], wkvsem.at[1])]
    def kv_copies(step):
        y_to = lax.rem(y_at + 1 + step, 4)
        pairs = []
        for r in range(2):
            rows = pl.ds(PLANE * r + 4 * y_to, 4)
            pairs.append(pltpu.make_async_copy(k_hbm.at[rows], kbuf.at[rows], ksem.at[2 * step + r]))
            pairs.append(pltpu.make_async_copy(v_hbm.at[rows], vbuf.at[rows], vsem.at[2 * step + r]))
        return pairs
    wo_copies = [pltpu.make_async_copy(
        wo_hbm.at[pl.ds(pl.multiple_of(my_half * K_HALF, K_HALF) + 192 * j, 192)], wobuf.at[pl.ds(192 * j, 192)],
        wsem.at[j]) for j in range(8)]

    vec_copies[0].wait()
    row_eye = lax.broadcasted_iota(jnp.int32, (N_ROWS, N_ROWS), 0) == lax.broadcasted_iota(jnp.int32, (N_ROWS, N_ROWS), 1)
    pos_col = jnp.sum(jnp.where(row_eye, pos_ref[...].astype(F32), 0.0), axis=1, keepdims=True)
    angles = pos_col * freq_ref[...]
    is_even = lax.rem(lax.broadcasted_iota(jnp.int32, (N_ROWS, D), 1), 2) == 0
    cos_t = jnp.cos(angles)
    sin_t = jnp.where(is_even, -jnp.sin(angles), jnp.sin(angles))

    def rotate(head):
        other = jnp.where(is_even, pltpu.roll(head, D - 1, 1), pltpu.roll(head, 1, 1))
        return (head * cos_t + other * sin_t).astype(BF16)

    hid_copy.wait()
    for cp in vec_copies[1:]:
        cp.wait()
    x_f32 = hid_ref[...].astype(F32)
    mean_sq = jnp.mean(x_f32 * x_f32, axis=-1, keepdims=True)
    unit = lax.rsqrt(mean_sq + RMS_EPS)
    nw_rows = nw_ref[...].astype(F32)
    for j in range(N_OUT // D):
        cut = slice(j * D, (j + 1) * D)
        normed[:, cut] = (x_f32[:, cut] * unit * nw_rows[j:j + 1, :]).astype(BF16)
    bq_rows[...] = bq_ref[...].astype(F32)

    q_mine = jnp.zeros((N_ROWS, Q_DEV), F32)
    for j, cp in enumerate(wq_copies):
        cp.wait()
        cut = slice(K_CUT * j, K_CUT * (j + 1))
        q_mine = q_mine + jnp.dot(normed[:, cut], wqbuf[cut, :], preferred_element_type=F32)
    for cp in wkv_copies:
        cp.start()
    for step in range(4):
        for cp in kv_copies(step):
            cp.start()
    for hf in range(2):
        q_all[pl.ds((hf * SLOT + HALF) * N_ROWS, (SLOT - HALF) * N_ROWS), :] = jnp.zeros(((SLOT - HALF) * N_ROWS, D), F32)

    def q_rows(lab):
        first = lax.div(lab, 4) * SLOT + 3 * lax.rem(lab, 4)
        return pl.multiple_of(first * N_ROWS, N_ROWS)
    for t in range(3):
        head = q_mine[:, t * D:(t + 1) * D] + bq_rows[pl.ds(3 * label + t, 1), :]
        q_all[pl.ds(q_rows(label) + t * N_ROWS, N_ROWS), :] = rotate(head.astype(BF16).astype(F32)).astype(F32)

    pl.semaphore_wait(barrier, SP + 1)

    def across(v):
        return lax.rem(v + 4 + (1 - 2 * lax.rem(v, 2)) * (1 - 2 * c), 4)
    q_copies = []
    for mask in range(7, 0, -1):
        zd = across(z) if mask & 4 else z
        yd = across(y_at) if mask & 2 else y_at
        xd = across(x_at) if mask & 1 else x_at
        mine = q_all.at[pl.ds(q_rows(label), 3 * N_ROWS)]
        q_copies.append(pltpu.make_async_remote_copy(
            src_ref=mine, dst_ref=mine, send_sem=q_send.at[mask - 1], recv_sem=q_recv.at[mask - 1],
            device_id={'sp': zd * PLANE + yd * 4 + xd}, device_id_type=MESH))
    for cp in q_copies:
        cp.start()

    for cp in wkv_copies:
        cp.wait()
    kv = jnp.dot(normed[...], wkvbuf[...], preferred_element_type=F32)
    k_new = rotate((kv[:, :D] + bk_ref[...].astype(F32)).astype(BF16).astype(F32))
    v_new = (kv[:, D:] + bv_ref[...].astype(F32)).astype(BF16)
    kn_rows[...] = k_new.astype(F32)
    vn_rows[...] = v_new.astype(F32)
    for step in range(4):
        for cp in kv_copies(step):
            cp.wait()
    for cp in wo_copies:
        cp.start()
    for cp in q_copies:
        cp.wait_recv()

    lane = lax.broadcasted_iota(jnp.int32, (SLOT, D), 1)
    sub = lax.broadcasted_iota(jnp.int32, (SLOT, D), 0)
    eye = lane == sub
    pos = s * S_DEV + lax.broadcasted_iota(jnp.int32, (2 * SLOT, S_DEV), 1)

    def rs_copy(dest):
        return pltpu.make_async_remote_copy(
            src_ref=o_send.at[dest], dst_ref=o_recv.at[pl.ds(pl.multiple_of(s * SLOT, SLOT), SLOT)],
            send_sem=rs_send, recv_sem=rs_recv, device_id={'sp': dest}, device_id_type=MESH)

    def rows_step(step, carry):
        y_to = lax.rem(y_at + 1 + step, 4)
        work = []
        for u in range(4):
            for r in range(2):
                chip = 4 * y_to + lax.rem(x_at + 1 + u, 4)
                work.append((u, r, chip, chip + PLANE * r))
        scores = []
        for u, r, chip, b in work:
            sc = lax.dot_general(q_all[pl.ds(b, 2 * SLOT, stride=N_ROWS), :].astype(BF16), kbuf[b],
                                 (((1,), (1,)), ((), ())), preferred_element_type=F32)
            scores.append(jnp.where(pos < seq_ref[b], sc, NEG_BIG))
        tops = [jnp.max(sc, axis=1, keepdims=True) for sc in scores]
        probs = [jnp.exp2((sc - m) * qk_scale) for sc, m in zip(scores, tops)]
        sums = [jnp.sum(pr, axis=1, keepdims=True) for pr in probs]
        for (u, r, chip, b), m, l, pr in zip(work, tops, sums, probs):
            o = jnp.dot(pr.astype(BF16), vbuf[b], preferred_element_type=F32)
            m2 = m * qk_scale
            for hf in range(2):
                part = slice(hf * SLOT, (hf + 1) * SLOT)
                m_row = jnp.sum(jnp.where(eye, m2[part], 0.0), axis=0, keepdims=True)
                l_row = jnp.sum(jnp.where(eye, l[part], 0.0), axis=0, keepdims=True)
                o_send[(2 * r + hf) * PLANE + chip] = jnp.where(
                    sub == HALF, m_row, jnp.where(sub == HALF + 1, l_row, o[part]))
        for u, r, chip, b in work:
            for hf in range(2):
                dest = (2 * r + hf) * PLANE + chip
                if u < 3:
                    rs_copy(dest).start()
                else:
                    @pl.when(dest != s)
                    def _():
                        rs_copy(dest).start()
        return carry
    lax.fori_loop(0, 4, rows_step, 0)
    mine = pl.ds(pl.multiple_of(s * SLOT, SLOT), SLOT)
    o_recv[mine, :] = o_send[s]

    my_row = p + PLANE * lax.div(z, 2)
    q_own = q_all[pl.ds(my_half * SLOT * N_ROWS + my_row, SLOT, stride=N_ROWS), :]
    k_mine = kn_rows[pl.ds(my_row, 1), :]
    v_mine = vn_rows[pl.ds(my_row, 1), :]
    s_new = jnp.sum(q_own * k_mine, axis=1, keepdims=True) * qk_scale

    def all_in(ref, sem):
        pltpu.make_async_copy(ref, ref, sem).wait()

    all_in(o_recv.at[pl.ds(0, (SP - 1) * SLOT)], rs_recv)
    m_rows = o_recv[pl.ds(HALF, SP, stride=SLOT), :]
    l_rows = o_recv[pl.ds(HALF + 1, SP, stride=SLOT), :]
    stats = jnp.transpose(jnp.concatenate([m_rows, l_rows], axis=0))[:SLOT]
    m_cols, l_cols = stats[:, :SP], stats[:, SP:]
    m_top = jnp.maximum(jnp.max(m_cols, axis=1, keepdims=True), s_new)
    w_cols = jnp.exp2(m_cols - m_top)
    w_new = jnp.exp2(s_new - m_top)
    l_all = jnp.sum(w_cols * l_cols, axis=1, keepdims=True) + w_new
    acc = w_new * v_mine
    for j in range(SP):
        acc = acc + w_cols[:, j:j + 1] * o_recv[j * SLOT:(j + 1) * SLOT, :]
    attn = acc / l_all
    lhs[...] = jnp.zeros_like(lhs)
    for j in range(HALF):
        lhs[0:1, j * D:(j + 1) * D] = attn[j:j + 1, :]
    for cp in wo_copies:
        cp.wait()

    lhs_b16 = lhs[...].astype(BF16)

    def product(half, place):
        for n in range(N_OUT // 2 // N_CUT):
            cols = pl.ds(pl.multiple_of(half * (N_OUT // 2) + n * N_CUT, N_CUT), N_CUT)
            piece = jnp.dot(lhs_b16, wobuf[:, cols], preferred_element_type=F32)
            for j in range(N_CUT // D):
                part[place, n * (N_CUT // D) + j:n * (N_CUT // D) + j + 1, :] = piece[0:1, j * D:(j + 1) * D]

    def x_copy(n, place, target):
        return pltpu.make_async_remote_copy(
            src_ref=part.at[place], dst_ref=others.at[n], send_sem=x_send.at[n], recv_sem=x_recv.at[n],
            device_id=target, device_id_type=MESH)
    x_copies = [x_copy(0, 1, {'sp': near, 'tp': 1 - c}), x_copy(1, 1, {'sp': near}), x_copy(2, 0, {'tp': 1 - c})]
    product(1 - my_half, 1)
    x_copies[0].start()
    x_copies[1].start()
    product(my_half, 0)
    x_copies[2].start()
    for cp in x_copies:
        cp.wait_recv()

    def ag_slot(i):
        return ag.at[pl.ds(pl.multiple_of(i * AG, 8), AG)]
    ag[pl.ds(pl.multiple_of(s * AG, 8), AG), :] = (part[0] + others[2]) + (others[0] + others[1])

    offsets = sorted(((dz, dy, j) for dz in range(4) for dy in range(4) for j in range(2)),
                     key=lambda d: min(d[0], 4 - d[0]) + min(d[1], 4 - d[1]) + 1.5 * d[2])

    def chip_at(dz, dy, dx):
        return lax.rem(z + dz, 4) * PLANE + lax.rem(y_at + dy, 4) * 4 + lax.rem(x_at + dx, 4)

    def ag_copy(n):
        dz, dy, j = offsets[n]
        return pltpu.make_async_remote_copy(
            src_ref=ag_slot(s), dst_ref=ag_slot(s), send_sem=ag_send, recv_sem=ag_recv.at[n],
            device_id={'sp': chip_at(dz, dy, 2 * j + c)}, device_id_type=MESH)

    def forward(n):
        dz, dy, j = offsets[n]
        slot = ag_slot(chip_at(4 - dz, 4 - dy, 4 - 2 * j - c))
        return slot, pltpu.make_async_remote_copy(
            src_ref=slot, dst_ref=slot, send_sem=f_send, recv_sem=f_recv, device_id={'tp': 1 - c}, device_id_type=MESH)

    def relay(n):
        slot, cp = forward(n)
        pltpu.make_async_copy(slot, slot, ag_recv.at[n]).wait()
        cp.start()

    def to_first_row(n):
        dz, dy, j = offsets[n]
        return jnp.logical_and(lax.rem(z + dz, 4) == 0, lax.rem(y_at + dy, 4) == 0)

    def ag_starts(wanted):
        for n in range(SP // 2 - 1, -1, -1):
            go = wanted(n) if n else jnp.logical_and(wanted(n), c == 1)

            @pl.when(go)
            def _():
                ag_copy(n).start()
    ag_starts(to_first_row)
    ag_starts(lambda n: jnp.logical_not(to_first_row(n)))

    @pl.when(c == 1)
    def _():
        relay(0)
    for n in range(1, SP // 2):
        relay(n)

    few, many = ag.at[pl.ds(0, (SP // 2 - 1) * AG)], ag.at[pl.ds(0, SP // 2 * AG)]

    @pl.when(c == 0)
    def _():
        all_in(many, f_recv)
        all_in(few, f_send)
        all_in(few, ag_send)

    @pl.when(c == 1)
    def _():
        all_in(few, f_recv)
        all_in(many, f_send)
        all_in(many, ag_send)
    all_in(o_send.at[pl.ds(0, SP - 1)], rs_send)
    for cp in q_copies + x_copies:
        cp.wait_send()


def step_call(freq, *operands):
    hidden, norm_w, w_q, b_q, w_k, b_k, w_v, b_v, w_o, k_cache, v_cache, positions, seq_lens = operands
    vmem = pl.BlockSpec(memory_space=pltpu.VMEM)
    hbm = pl.BlockSpec(memory_space=pltpu.HBM)
    dma = pltpu.SemaphoreType.DMA
    return pl.pallas_call(
        step_kernel,
        out_shape=(jax.ShapeDtypeStruct((SP * AG, D), F32),
                   jax.ShapeDtypeStruct((N_ROWS, D), F32), jax.ShapeDtypeStruct((N_ROWS, D), F32)),
        in_specs=[hbm, hbm, hbm, hbm, hbm, vmem, hbm, hbm, hbm, hbm, hbm, hbm, hbm, hbm],
        out_specs=(vmem, vmem, vmem),
        scratch_shapes=[
            pltpu.VMEM((N_OUT // D, D), BF16),
            pltpu.VMEM((24, D), BF16),
            pltpu.VMEM((1, D), BF16),
            pltpu.VMEM((1, D), BF16),
            pltpu.VMEM((1, N_ROWS), jnp.int32),
            pltpu.SMEM((N_ROWS,), jnp.int32),
            pltpu.VMEM((N_ROWS, N_OUT), BF16),
            pltpu.VMEM((N_ROWS, N_OUT), BF16),
            pltpu.VMEM((N_OUT, Q_DEV), BF16),
            pltpu.VMEM((N_OUT, 2 * D), BF16),
            pltpu.VMEM((24, D), F32),
            pltpu.VMEM((2 * SLOT * N_ROWS, D), F32),
            pltpu.VMEM((N_ROWS, S_DEV, D), BF16),
            pltpu.VMEM((N_ROWS, S_DEV, D), BF16),
            pltpu.VMEM((K_HALF, N_OUT), BF16),
            pltpu.VMEM((2 * N_ROWS, SLOT, D), F32),
            pltpu.VMEM((SP * SLOT, D), F32),
            pltpu.VMEM((8, K_HALF), F32),
            pltpu.VMEM((2, AG, D), F32),
            pltpu.VMEM((3, AG, D), F32),
            dma((6,)), dma, dma((N_OUT // K_CUT,)), dma((2,)), dma((7,)), dma((7,)),
            dma((8,)), dma((8,)), dma((8,)), dma, dma, dma((3,)), dma((3,)),
            dma, dma((SP // 2,)), dma, dma,
        ],
        compiler_params=pltpu.CompilerParams(
            collective_id=0, has_side_effects=True, vmem_limit_bytes=44 * 1024 * 1024),
        name='decode_step',
    )(*(x if x is freq else pltpu.with_memory_space_constraint(x, pltpu.HBM) for x in (
        hidden, norm_w.reshape(-1, D), b_q.reshape(-1, D), b_k.reshape(1, -1), b_v.reshape(1, -1), freq,
        positions.reshape(1, -1), seq_lens, w_q, w_k, w_v,
        k_cache.reshape(N_ROWS, S_DEV, D), v_cache.reshape(N_ROWS, S_DEV, D), w_o)))


def finish_kernel(ag, kn_rows, vn_rows, hid_ref, y_ref, kn_ref, vn_ref):
    kn_ref[...] = kn_rows[...].astype(BF16)
    vn_ref[...] = vn_rows[...].astype(BF16)
    for zz in range(4):
        r, hf = zz // 2, zz % 2
        rows = slice(PLANE * r, PLANE * (r + 1))
        for blk in range(AG):
            col = slice(hf * (N_OUT // 2) + blk * D, hf * (N_OUT // 2) + (blk + 1) * D)
            y_blk = ag[pl.ds(zz * PLANE * AG + blk, PLANE, stride=AG), :]
            y_ref[rows, col] = (hid_ref[rows, col].astype(F32) + y_blk).astype(BF16)


def finish(ag, kn_rows, vn_rows, hidden):
    vmem = pl.BlockSpec(memory_space=pltpu.VMEM)
    return pl.pallas_call(
        finish_kernel,
        out_shape=(jax.ShapeDtypeStruct((N_ROWS, N_OUT), BF16),
                   jax.ShapeDtypeStruct((N_ROWS, D), BF16), jax.ShapeDtypeStruct((N_ROWS, D), BF16)),
        in_specs=[vmem] * 4, out_specs=(vmem,) * 3,
        compiler_params=pltpu.CompilerParams(vmem_limit_bytes=8 * 1024 * 1024),
        name='finish',
    )(ag, kn_rows, vn_rows, hidden)


def solution(mesh):
    def device_step(*operands):
        lane = jnp.arange(D, dtype=jnp.int32)
        inv_freq = ROPE_BASE ** (-2.0 * (lane // 2).astype(jnp.float32) / (D // 2))
        freq = jnp.where(lane < D // 2, inv_freq, 0.0).reshape(1, D)
        y_out, k_new, v_new = finish(*step_call(freq, *operands), operands[0])
        return y_out, k_new.reshape(N_ROWS, 1, D), v_new.reshape(N_ROWS, 1, D)

    col_spec = P(None, 'tp')
    vec_spec = P('tp')
    cache_spec = P('dp', 'sp', 'tp', None)
    group_spec = P('dp', 'tp', None)
    in_specs = (P('dp', None), P(None), col_spec, vec_spec, col_spec, vec_spec, col_spec, vec_spec,
                P('tp', None), cache_spec, cache_spec, P('dp'), P('dp'))
    out_specs = (P('dp', None), group_spec, group_spec)
    return jax.shard_map(device_step, mesh=mesh, in_specs=in_specs, out_specs=out_specs, check_vma=False)
```

```python
import functools
import math

import jax
import jax.numpy as jnp
from jax import lax
from jax.experimental import pallas as pl
from jax.experimental.pallas import tpu as pltpu
from jax.sharding import PartitionSpec as P

RMS_EPS = 1.5625e-7
ROPE_BASE = 10000.0
NEG_BIG = -3.0e38
MESH = pl.DeviceIdType.MESH
F32 = jnp.float32
BF16 = jnp.bfloat16

N_ROWS = 32
S_DEV = 512
D = 128
SP = 64
PLANE = 16
HALF = 12
SLOT = 16
N_OUT = 6144
K_HALF = 1536
N_CUT = 1024
AG = 24
Q_DEV = 384
K_CUT = 1536


def step_kernel(hid_hbm, nw_hbm, bq_hbm, bk_hbm, bv_hbm, freq_ref, pos_hbm, seq_hbm,
                wq_hbm, wk_hbm, wv_hbm, k_hbm, v_hbm, wo_hbm, ag, kn_rows, vn_rows,
                nw_ref, bq_ref, bk_ref, bv_ref, pos_ref, seq_ref, hid_ref, normed, wqbuf, wkvbuf, bq_rows, q_all,
                kbuf, vbuf, wobuf, o_send, o_recv, lhs, part, others,
                vecsem, hsem, wqsem, wkvsem, q_send, q_recv,
                ksem, vsem, wsem, rs_send, rs_recv, x_send, x_recv,
                ag_send, ag_recv, f_send, f_recv):
    c = lax.axis_index('tp')
    s = lax.axis_index('sp')
    z = lax.div(s, PLANE)
    p = lax.rem(s, PLANE)
    y_at = lax.div(p, 4)
    x_at = lax.rem(p, 4)
    qk_scale = (D ** -0.5) * math.log2(math.e)

    def chip_at(dz, dy, dx):
        return lax.rem(z + dz, 4) * PLANE + lax.rem(y_at + dy, 4) * 4 + lax.rem(x_at + dx, 4)

    barrier = pltpu.get_barrier_semaphore()
    far_first = sorted(((dz, dy, dx) for dz in range(4) for dy in range(4) for dx in range(4)),
                       key=lambda d: -sum(min(v, 4 - v) for v in d))[:-1]
    for dz, dy, dx in far_first:
        pl.semaphore_signal(barrier, inc=1, device_id={'sp': chip_at(dz, dy, dx)}, device_id_type=MESH)
    pl.semaphore_signal(barrier, inc=1, device_id={'tp': 1 - c}, device_id_type=MESH)
    my_half = lax.rem(z, 2)
    near = (z + 1 - 2 * my_half) * PLANE + p
    pl.semaphore_signal(barrier, inc=1, device_id={'sp': near, 'tp': 1 - c}, device_id_type=MESH)

    wkv_copies = [pltpu.make_async_copy(wk_hbm, wkvbuf.at[:, pl.ds(0, D)], wkvsem.at[0]),
                  pltpu.make_async_copy(wv_hbm, wkvbuf.at[:, pl.ds(D, D)], wkvsem.at[1])]
    label = 4 * lax.rem(z, 2) + 2 * lax.rem(y_at, 2) + lax.rem(x_at, 2)
    hid_copy = pltpu.make_async_copy(hid_hbm, hid_ref, hsem)
    hid_copy.start()
    vec_copies = [pltpu.make_async_copy(src, dst, vecsem.at[j]) for j, (src, dst) in enumerate((
        (pos_hbm, pos_ref), (nw_hbm, nw_ref), (bq_hbm, bq_ref), (bk_hbm, bk_ref), (bv_hbm, bv_ref), (seq_hbm, seq_ref)))]
    for cp in vec_copies:
        cp.start()
    q_cols = pl.ds(pl.multiple_of(label * Q_DEV, D), Q_DEV)
    wq_copies = [pltpu.make_async_copy(
        wq_hbm.at[pl.ds(K_CUT * j, K_CUT), q_cols], wqbuf.at[pl.ds(K_CUT * j, K_CUT)], wqsem.at[j])
        for j in range(N_OUT // K_CUT)]
    for cp in wq_copies:
        cp.start()

    def kv_copies(step):
        y_to = lax.rem(y_at + 1 + step, 4)
        pairs = []
        for r in range(2):
            rows = pl.ds(PLANE * r + 4 * y_to, 4)
            pairs.append(pltpu.make_async_copy(k_hbm.at[rows], kbuf.at[rows], ksem.at[2 * step + r]))
            pairs.append(pltpu.make_async_copy(v_hbm.at[rows], vbuf.at[rows], vsem.at[2 * step + r]))
        return pairs
    wo_copies = [pltpu.make_async_copy(
        wo_hbm.at[pl.ds(pl.multiple_of(my_half * K_HALF, K_HALF) + 192 * j, 192)], wobuf.at[pl.ds(192 * j, 192)],
        wsem.at[j]) for j in range(8)]

    vec_copies[0].wait()
    row_eye = lax.broadcasted_iota(jnp.int32, (N_ROWS, N_ROWS), 0) == lax.broadcasted_iota(jnp.int32, (N_ROWS, N_ROWS), 1)
    pos_col = jnp.sum(jnp.where(row_eye, pos_ref[...].astype(F32), 0.0), axis=1, keepdims=True)
    angles = pos_col * freq_ref[...]
    is_even = lax.rem(lax.broadcasted_iota(jnp.int32, (N_ROWS, D), 1), 2) == 0
    cos_t = jnp.cos(angles)
    sin_t = jnp.where(is_even, -jnp.sin(angles), jnp.sin(angles))

    def rotate(head):
        other = jnp.where(is_even, pltpu.roll(head, D - 1, 1), pltpu.roll(head, 1, 1))
        return (head * cos_t + other * sin_t).astype(BF16)

    hid_copy.wait()
    for cp in vec_copies[1:]:
        cp.wait()
    x_f32 = hid_ref[...].astype(F32)
    mean_sq = jnp.mean(x_f32 * x_f32, axis=-1, keepdims=True)
    unit = lax.rsqrt(mean_sq + RMS_EPS)
    nw_rows = nw_ref[...].astype(F32)
    for j in range(N_OUT // D):
        cut = slice(j * D, (j + 1) * D)
        normed[:, cut] = (x_f32[:, cut] * unit * nw_rows[j:j + 1, :]).astype(BF16)
    bq_rows[...] = bq_ref[...].astype(F32)

    q_mine = jnp.zeros((N_ROWS, Q_DEV), F32)
    for j, cp in enumerate(wq_copies):
        cp.wait()
        cut = slice(K_CUT * j, K_CUT * (j + 1))
        q_mine = q_mine + jnp.dot(normed[:, cut], wqbuf[cut, :], preferred_element_type=F32)
    for cp in wkv_copies:
        cp.start()
    for step in range(4):
        for cp in kv_copies(step):
            cp.start()
    for hf in range(2):
        q_all[pl.ds((hf * SLOT + HALF) * N_ROWS, (SLOT - HALF) * N_ROWS), :] = jnp.zeros(((SLOT - HALF) * N_ROWS, D), F32)

    def q_rows(lab):
        first = lax.div(lab, 4) * SLOT + 3 * lax.rem(lab, 4)
        return pl.multiple_of(first * N_ROWS, N_ROWS)
    for t in range(3):
        head = q_mine[:, t * D:(t + 1) * D] + bq_rows[pl.ds(3 * label + t, 1), :]
        q_all[pl.ds(q_rows(label) + t * N_ROWS, N_ROWS), :] = rotate(head.astype(BF16).astype(F32)).astype(F32)

    pl.semaphore_wait(barrier, SP + 1)

    def across(v):
        return lax.rem(v + 4 + (1 - 2 * lax.rem(v, 2)) * (1 - 2 * c), 4)
    q_copies = []
    for mask in range(7, 0, -1):
        zd = across(z) if mask & 4 else z
        yd = across(y_at) if mask & 2 else y_at
        xd = across(x_at) if mask & 1 else x_at
        mine = q_all.at[pl.ds(q_rows(label), 3 * N_ROWS)]
        q_copies.append(pltpu.make_async_remote_copy(
            src_ref=mine, dst_ref=mine, send_sem=q_send.at[mask - 1], recv_sem=q_recv.at[mask - 1],
            device_id={'sp': zd * PLANE + yd * 4 + xd}, device_id_type=MESH))
    for cp in q_copies:
        cp.start()

    for cp in wkv_copies:
        cp.wait()
    kv = jnp.dot(normed[...], wkvbuf[...], preferred_element_type=F32)
    k_new = rotate((kv[:, :D] + bk_ref[...].astype(F32)).astype(BF16).astype(F32))
    v_new = (kv[:, D:] + bv_ref[...].astype(F32)).astype(BF16)
    kn_rows[...] = k_new.astype(F32)
    vn_rows[...] = v_new.astype(F32)
    for step in range(4):
        for cp in kv_copies(step):
            cp.wait()
    for cp in wo_copies:
        cp.start()
    for cp in q_copies:
        cp.wait_recv()

    lane = lax.broadcasted_iota(jnp.int32, (SLOT, D), 1)
    sub = lax.broadcasted_iota(jnp.int32, (SLOT, D), 0)
    eye = lane == sub
    pos = s * S_DEV + lax.broadcasted_iota(jnp.int32, (2 * SLOT, S_DEV), 1)

    def rs_copy(dest):
        return pltpu.make_async_remote_copy(
            src_ref=o_send.at[dest], dst_ref=o_recv.at[pl.ds(pl.multiple_of(s * SLOT, SLOT), SLOT)],
            send_sem=rs_send, recv_sem=rs_recv, device_id={'sp': dest}, device_id_type=MESH)

    def rows_step(step, carry):
        y_to = lax.rem(y_at + 1 + step, 4)
        work = []
        for u in range(4):
            for r in range(2):
                chip = 4 * y_to + lax.rem(x_at + 1 + u, 4)
                work.append((u, r, chip, chip + PLANE * r))
        scores = []
        for u, r, chip, b in work:
            sc = lax.dot_general(q_all[pl.ds(b, 2 * SLOT, stride=N_ROWS), :].astype(BF16), kbuf[b],
                                 (((1,), (1,)), ((), ())), preferred_element_type=F32)
            scores.append(jnp.where(pos < seq_ref[b], sc, NEG_BIG))
        tops = [jnp.max(sc, axis=1, keepdims=True) for sc in scores]
        probs = [jnp.exp2((sc - m) * qk_scale) for sc, m in zip(scores, tops)]
        sums = [jnp.sum(pr, axis=1, keepdims=True) for pr in probs]
        for (u, r, chip, b), m, l, pr in zip(work, tops, sums, probs):
            o = jnp.dot(pr.astype(BF16), vbuf[b], preferred_element_type=F32)
            m2 = m * qk_scale
            for hf in range(2):
                part = slice(hf * SLOT, (hf + 1) * SLOT)
                m_row = jnp.sum(jnp.where(eye, m2[part], 0.0), axis=0, keepdims=True)
                l_row = jnp.sum(jnp.where(eye, l[part], 0.0), axis=0, keepdims=True)
                o_send[(2 * r + hf) * PLANE + chip] = jnp.where(
                    sub == HALF, m_row, jnp.where(sub == HALF + 1, l_row, o[part]))
        for u, r, chip, b in work:
            for hf in range(2):
                dest = (2 * r + hf) * PLANE + chip
                if u < 3:
                    rs_copy(dest).start()
                else:
                    @pl.when(dest != s)
                    def _():
                        rs_copy(dest).start()
        return carry
    lax.fori_loop(0, 4, rows_step, 0)
    mine = pl.ds(pl.multiple_of(s * SLOT, SLOT), SLOT)
    o_recv[mine, :] = o_send[s]

    my_row = p + PLANE * lax.div(z, 2)
    q_own = q_all[pl.ds(my_half * SLOT * N_ROWS + my_row, SLOT, stride=N_ROWS), :]
    k_mine = kn_rows[pl.ds(my_row, 1), :]
    v_mine = vn_rows[pl.ds(my_row, 1), :]
    s_new = jnp.sum(q_own * k_mine, axis=1, keepdims=True) * qk_scale

    def all_in(ref, sem):
        pltpu.make_async_copy(ref, ref, sem).wait()

    all_in(o_recv.at[pl.ds(0, (SP - 1) * SLOT)], rs_recv)
    m_rows = o_recv[pl.ds(HALF, SP, stride=SLOT), :]
    l_rows = o_recv[pl.ds(HALF + 1, SP, stride=SLOT), :]
    stats = jnp.transpose(jnp.concatenate([m_rows, l_rows], axis=0))[:SLOT]
    m_cols, l_cols = stats[:, :SP], stats[:, SP:]
    m_top = jnp.maximum(jnp.max(m_cols, axis=1, keepdims=True), s_new)
    w_cols = jnp.exp2(m_cols - m_top)
    w_new = jnp.exp2(s_new - m_top)
    l_all = jnp.sum(w_cols * l_cols, axis=1, keepdims=True) + w_new
    acc = w_new * v_mine
    for j in range(SP):
        acc = acc + w_cols[:, j:j + 1] * o_recv[j * SLOT:(j + 1) * SLOT, :]
    attn = acc / l_all
    lhs[...] = jnp.zeros_like(lhs)
    for j in range(HALF):
        lhs[0:1, j * D:(j + 1) * D] = attn[j:j + 1, :]
    for cp in wo_copies:
        cp.wait()

    lhs_b16 = lhs[...].astype(BF16)

    def product(half, place):
        for n in range(N_OUT // 2 // N_CUT):
            cols = pl.ds(pl.multiple_of(half * (N_OUT // 2) + n * N_CUT, N_CUT), N_CUT)
            piece = jnp.dot(lhs_b16, wobuf[:, cols], preferred_element_type=F32)
            for j in range(N_CUT // D):
                part[place, n * (N_CUT // D) + j:n * (N_CUT // D) + j + 1, :] = piece[0:1, j * D:(j + 1) * D]

    def x_copy(n, place, target):
        return pltpu.make_async_remote_copy(
            src_ref=part.at[place], dst_ref=others.at[n], send_sem=x_send.at[n], recv_sem=x_recv.at[n],
            device_id=target, device_id_type=MESH)
    x_copies = [x_copy(0, 1, {'sp': near, 'tp': 1 - c}), x_copy(1, 1, {'sp': near}), x_copy(2, 0, {'tp': 1 - c})]
    product(1 - my_half, 1)
    x_copies[0].start()
    x_copies[1].start()
    product(my_half, 0)
    x_copies[2].start()
    for cp in x_copies:
        cp.wait_recv()

    def ag_slot(i):
        return ag.at[pl.ds(pl.multiple_of(i * AG, 8), AG)]
    ag[pl.ds(pl.multiple_of(s * AG, 8), AG), :] = (part[0] + others[2]) + (others[0] + others[1])

    offsets = sorted(((dz, dy, j) for dz in range(4) for dy in range(4) for j in range(2)),
                     key=lambda d: min(d[0], 4 - d[0]) + min(d[1], 4 - d[1]) + 1.5 * d[2])

    def ag_copy(n):
        dz, dy, j = offsets[n]
        return pltpu.make_async_remote_copy(
            src_ref=ag_slot(s), dst_ref=ag_slot(s), send_sem=ag_send, recv_sem=ag_recv.at[n],
            device_id={'sp': chip_at(dz, dy, 2 * j + c)}, device_id_type=MESH)

    def forward(n):
        dz, dy, j = offsets[n]
        slot = ag_slot(chip_at(4 - dz, 4 - dy, 4 - 2 * j - c))
        return slot, pltpu.make_async_remote_copy(
            src_ref=slot, dst_ref=slot, send_sem=f_send, recv_sem=f_recv, device_id={'tp': 1 - c}, device_id_type=MESH)

    def relay(n):
        slot, cp = forward(n)
        pltpu.make_async_copy(slot, slot, ag_recv.at[n]).wait()
        cp.start()

    def to_first_row(n):
        dz, dy, j = offsets[n]
        return jnp.logical_and(lax.rem(z + dz, 4) == 0, lax.rem(y_at + dy, 4) == 0)

    def ag_starts(wanted):
        for n in range(SP // 2 - 1, -1, -1):
            go = wanted(n) if n else jnp.logical_and(wanted(n), c == 1)

            @pl.when(go)
            def _():
                ag_copy(n).start()
    ag_starts(to_first_row)
    ag_starts(lambda n: jnp.logical_not(to_first_row(n)))

    @pl.when(c == 1)
    def _():
        relay(0)
    for n in range(1, SP // 2):
        relay(n)

    few, many = ag.at[pl.ds(0, (SP // 2 - 1) * AG)], ag.at[pl.ds(0, SP // 2 * AG)]

    @pl.when(c == 0)
    def _():
        all_in(many, f_recv)
        all_in(few, f_send)
        all_in(few, ag_send)

    @pl.when(c == 1)
    def _():
        all_in(few, f_recv)
        all_in(many, f_send)
        all_in(many, ag_send)
    all_in(o_send.at[pl.ds(0, SP - 1)], rs_send)
    for cp in q_copies + x_copies:
        cp.wait_send()


def step_call(freq, *operands):
    hidden, norm_w, w_q, b_q, w_k, b_k, w_v, b_v, w_o, k_cache, v_cache, positions, seq_lens = operands
    vmem = pl.BlockSpec(memory_space=pltpu.VMEM)
    hbm = pl.BlockSpec(memory_space=pltpu.HBM)
    dma = pltpu.SemaphoreType.DMA
    return pl.pallas_call(
        step_kernel,
        out_shape=(jax.ShapeDtypeStruct((SP * AG, D), F32),
                   jax.ShapeDtypeStruct((N_ROWS, D), F32), jax.ShapeDtypeStruct((N_ROWS, D), F32)),
        in_specs=[hbm, hbm, hbm, hbm, hbm, vmem, hbm, hbm, hbm, hbm, hbm, hbm, hbm, hbm],
        out_specs=(vmem, vmem, vmem),
        scratch_shapes=[
            pltpu.VMEM((N_OUT // D, D), BF16),
            pltpu.VMEM((24, D), BF16),
            pltpu.VMEM((1, D), BF16),
            pltpu.VMEM((1, D), BF16),
            pltpu.VMEM((1, N_ROWS), jnp.int32),
            pltpu.SMEM((N_ROWS,), jnp.int32),
            pltpu.VMEM((N_ROWS, N_OUT), BF16),
            pltpu.VMEM((N_ROWS, N_OUT), BF16),
            pltpu.VMEM((N_OUT, Q_DEV), BF16),
            pltpu.VMEM((N_OUT, 2 * D), BF16),
            pltpu.VMEM((24, D), F32),
            pltpu.VMEM((2 * SLOT * N_ROWS, D), F32),
            pltpu.VMEM((N_ROWS, S_DEV, D), BF16),
            pltpu.VMEM((N_ROWS, S_DEV, D), BF16),
            pltpu.VMEM((K_HALF, N_OUT), BF16),
            pltpu.VMEM((2 * N_ROWS, SLOT, D), F32),
            pltpu.VMEM((SP * SLOT, D), F32),
            pltpu.VMEM((8, K_HALF), F32),
            pltpu.VMEM((2, AG, D), F32),
            pltpu.VMEM((3, AG, D), F32),
            dma((6,)), dma, dma((N_OUT // K_CUT,)), dma((2,)), dma((7,)), dma((7,)),
            dma((8,)), dma((8,)), dma((8,)), dma, dma, dma((3,)), dma((3,)),
            dma, dma((SP // 2,)), dma, dma,
        ],
        compiler_params=pltpu.CompilerParams(
            collective_id=0, has_side_effects=True, vmem_limit_bytes=44 * 1024 * 1024),
        name='decode_step',
    )(*(x if x is freq else pltpu.with_memory_space_constraint(x, pltpu.HBM) for x in (
        hidden, norm_w.reshape(-1, D), b_q.reshape(-1, D), b_k.reshape(1, -1), b_v.reshape(1, -1), freq,
        positions.reshape(1, -1), seq_lens, w_q, w_k, w_v,
        k_cache.reshape(N_ROWS, S_DEV, D), v_cache.reshape(N_ROWS, S_DEV, D), w_o)))


def finish_kernel(ag, kn_rows, vn_rows, hid_ref, y_hbm, kn_hbm, vn_hbm, y_ref, kn_ref, vn_ref, sems):
    kn_ref[...] = kn_rows[...].astype(BF16)
    vn_ref[...] = vn_rows[...].astype(BF16)
    copies = [pltpu.make_async_copy(kn_ref, kn_hbm, sems.at[0]), pltpu.make_async_copy(vn_ref, vn_hbm, sems.at[1])]
    for zz in range(4):
        r, hf = zz // 2, zz % 2
        rows = slice(PLANE * r, PLANE * (r + 1))
        for blk in range(AG):
            col = slice(hf * (N_OUT // 2) + blk * D, hf * (N_OUT // 2) + (blk + 1) * D)
            y_blk = ag[pl.ds(zz * PLANE * AG + blk, PLANE, stride=AG), :]
            y_ref[rows, col] = (hid_ref[rows, col].astype(F32) + y_blk).astype(BF16)
        block = (pl.ds(PLANE * r, PLANE), pl.ds(hf * (N_OUT // 2), N_OUT // 2))
        copies.append(pltpu.make_async_copy(y_ref.at[block], y_hbm.at[block], sems.at[2 + zz]))
        if zz == 0:
            copies[0].start()
            copies[1].start()
        copies[-1].start()
    for cp in copies:
        cp.wait()


def finish(ag, kn_rows, vn_rows, hidden):
    vmem = pl.BlockSpec(memory_space=pltpu.VMEM)
    hbm = pl.BlockSpec(memory_space=pltpu.HBM)
    return pl.pallas_call(
        finish_kernel,
        out_shape=(jax.ShapeDtypeStruct((N_ROWS, N_OUT), BF16),
                   jax.ShapeDtypeStruct((N_ROWS, D), BF16), jax.ShapeDtypeStruct((N_ROWS, D), BF16)),
        in_specs=[vmem] * 4, out_specs=(hbm,) * 3,
        scratch_shapes=[pltpu.VMEM((N_ROWS, N_OUT), BF16), pltpu.VMEM((N_ROWS, D), BF16),
                        pltpu.VMEM((N_ROWS, D), BF16), pltpu.SemaphoreType.DMA((6,))],
        compiler_params=pltpu.CompilerParams(vmem_limit_bytes=8 * 1024 * 1024),
        name='finish',
    )(ag, kn_rows, vn_rows, hidden)


def solution(mesh):
    def device_step(*operands):
        lane = jnp.arange(D, dtype=jnp.int32)
        inv_freq = ROPE_BASE ** (-2.0 * (lane // 2).astype(jnp.float32) / (D // 2))
        freq = jnp.where(lane < D // 2, inv_freq, 0.0).reshape(1, D)
        y_out, k_new, v_new = finish(*step_call(freq, *operands), operands[0])
        return y_out, k_new.reshape(N_ROWS, 1, D), v_new.reshape(N_ROWS, 1, D)

    col_spec = P(None, 'tp')
    vec_spec = P('tp')
    cache_spec = P('dp', 'sp', 'tp', None)
    group_spec = P('dp', 'tp', None)
    in_specs = (P('dp', None), P(None), col_spec, vec_spec, col_spec, vec_spec, col_spec, vec_spec,
                P('tp', None), cache_spec, cache_spec, P('dp'), P('dp'))
    out_specs = (P('dp', None), group_spec, group_spec)
    return jax.shard_map(device_step, mesh=mesh, in_specs=in_specs, out_specs=out_specs, check_vma=False)
```

```python
import functools
import math

import jax
import jax.numpy as jnp
from jax import lax
from jax.experimental import pallas as pl
from jax.experimental.pallas import tpu as pltpu
from jax.sharding import PartitionSpec as P

RMS_EPS = 1.5625e-7
ROPE_BASE = 10000.0
NEG_BIG = -3.0e38
MESH = pl.DeviceIdType.MESH
F32 = jnp.float32
BF16 = jnp.bfloat16

N_ROWS = 32
S_DEV = 512
D = 128
SP = 64
PLANE = 16
HALF = 12
SLOT = 16
N_OUT = 6144
K_HALF = 1536
N_CUT = 1024
AG = 24
Q_DEV = 384
K_CUT = 1536


def step_kernel(hid_hbm, nw_hbm, bq_hbm, bk_hbm, bv_hbm, freq_ref, pos_hbm, seq_hbm,
                wq_hbm, wk_hbm, wv_hbm, k_hbm, v_hbm, wo_hbm, ag, kn_rows, vn_rows,
                nw_ref, bq_ref, bk_ref, bv_ref, pos_ref, seq_ref, hid_ref, normed, wqbuf, wkvbuf, bq_rows, q_all,
                kbuf, vbuf, wobuf, o_send, o_recv, lhs, part, others,
                vecsem, hsem, wqsem, wkvsem, q_send, q_recv,
                ksem, vsem, wsem, rs_send, rs_recv, x_send, x_recv,
                ag_send, ag_recv, f_send, f_recv):
    c = lax.axis_index('tp')
    s = lax.axis_index('sp')
    z = lax.div(s, PLANE)
    p = lax.rem(s, PLANE)
    y_at = lax.div(p, 4)
    x_at = lax.rem(p, 4)
    qk_scale = (D ** -0.5) * math.log2(math.e)

    def chip_at(dz, dy, dx):
        return lax.rem(z + dz, 4) * PLANE + lax.rem(y_at + dy, 4) * 4 + lax.rem(x_at + dx, 4)

    barrier = pltpu.get_barrier_semaphore()
    far_first = sorted(((dz, dy, dx) for dz in range(4) for dy in range(4) for dx in range(4)),
                       key=lambda d: -sum(min(v, 4 - v) for v in d))[:-1]
    for dz, dy, dx in far_first:
        pl.semaphore_signal(barrier, inc=1, device_id={'sp': chip_at(dz, dy, dx)}, device_id_type=MESH)
    pl.semaphore_signal(barrier, inc=1, device_id={'tp': 1 - c}, device_id_type=MESH)
    my_half = lax.rem(z, 2)
    near = (z + 1 - 2 * my_half) * PLANE + p
    pl.semaphore_signal(barrier, inc=1, device_id={'sp': near, 'tp': 1 - c}, device_id_type=MESH)

    wkv_copies = [pltpu.make_async_copy(wk_hbm, wkvbuf.at[:, pl.ds(0, D)], wkvsem.at[0]),
                  pltpu.make_async_copy(wv_hbm, wkvbuf.at[:, pl.ds(D, D)], wkvsem.at[1])]
    label = 4 * lax.rem(z, 2) + 2 * lax.rem(y_at, 2) + lax.rem(x_at, 2)
    hid_copy = pltpu.make_async_copy(hid_hbm, hid_ref, hsem)
    hid_copy.start()
    vec_copies = [pltpu.make_async_copy(src, dst, vecsem.at[j]) for j, (src, dst) in enumerate((
        (pos_hbm, pos_ref), (nw_hbm, nw_ref), (bq_hbm, bq_ref), (bk_hbm, bk_ref), (bv_hbm, bv_ref), (seq_hbm, seq_ref)))]
    for cp in vec_copies:
        cp.start()
    q_cols = pl.ds(pl.multiple_of(label * Q_DEV, D), Q_DEV)
    wq_copies = [pltpu.make_async_copy(
        wq_hbm.at[pl.ds(K_CUT * j, K_CUT), q_cols], wqbuf.at[pl.ds(K_CUT * j, K_CUT)], wqsem.at[j])
        for j in range(N_OUT // K_CUT)]
    for cp in wq_copies:
        cp.start()

    def far_rows(step):
        return jnp.where(step == 0, 2, jnp.where(step == 1, 1, jnp.where(step == 2, 3, 0)))

    def kv_copies(step):
        y_to = lax.rem(y_at + far_rows(step), 4)
        pairs = []
        for r in range(2):
            rows = pl.ds(PLANE * r + 4 * y_to, 4)
            pairs.append(pltpu.make_async_copy(k_hbm.at[rows], kbuf.at[rows], ksem.at[2 * step + r]))
            pairs.append(pltpu.make_async_copy(v_hbm.at[rows], vbuf.at[rows], vsem.at[2 * step + r]))
        return pairs
    wo_copies = [pltpu.make_async_copy(
        wo_hbm.at[pl.ds(pl.multiple_of(my_half * K_HALF, K_HALF) + 192 * j, 192)], wobuf.at[pl.ds(192 * j, 192)],
        wsem.at[j]) for j in range(8)]

    vec_copies[0].wait()
    row_eye = lax.broadcasted_iota(jnp.int32, (N_ROWS, N_ROWS), 0) == lax.broadcasted_iota(jnp.int32, (N_ROWS, N_ROWS), 1)
    pos_col = jnp.sum(jnp.where(row_eye, pos_ref[...].astype(F32), 0.0), axis=1, keepdims=True)
    angles = pos_col * freq_ref[...]
    is_even = lax.rem(lax.broadcasted_iota(jnp.int32, (N_ROWS, D), 1), 2) == 0
    cos_t = jnp.cos(angles)
    sin_t = jnp.where(is_even, -jnp.sin(angles), jnp.sin(angles))

    def rotate(head):
        other = jnp.where(is_even, pltpu.roll(head, D - 1, 1), pltpu.roll(head, 1, 1))
        return (head * cos_t + other * sin_t).astype(BF16)

    hid_copy.wait()
    for cp in vec_copies[1:]:
        cp.wait()
    x_f32 = hid_ref[...].astype(F32)
    mean_sq = jnp.mean(x_f32 * x_f32, axis=-1, keepdims=True)
    unit = lax.rsqrt(mean_sq + RMS_EPS)
    nw_rows = nw_ref[...].astype(F32)
    for j in range(N_OUT // D):
        cut = slice(j * D, (j + 1) * D)
        normed[:, cut] = (x_f32[:, cut] * unit * nw_rows[j:j + 1, :]).astype(BF16)
    bq_rows[...] = bq_ref[...].astype(F32)

    q_mine = jnp.zeros((N_ROWS, Q_DEV), F32)
    for j, cp in enumerate(wq_copies):
        cp.wait()
        cut = slice(K_CUT * j, K_CUT * (j + 1))
        q_mine = q_mine + jnp.dot(normed[:, cut], wqbuf[cut, :], preferred_element_type=F32)
    for cp in wkv_copies:
        cp.start()
    for step in range(4):
        for cp in kv_copies(step):
            cp.start()
    for hf in range(2):
        q_all[pl.ds((hf * SLOT + HALF) * N_ROWS, (SLOT - HALF) * N_ROWS), :] = jnp.zeros(((SLOT - HALF) * N_ROWS, D), F32)

    def q_rows(lab):
        first = lax.div(lab, 4) * SLOT + 3 * lax.rem(lab, 4)
        return pl.multiple_of(first * N_ROWS, N_ROWS)
    for t in range(3):
        head = q_mine[:, t * D:(t + 1) * D] + bq_rows[pl.ds(3 * label + t, 1), :]
        q_all[pl.ds(q_rows(label) + t * N_ROWS, N_ROWS), :] = rotate(head.astype(BF16).astype(F32)).astype(F32)

    pl.semaphore_wait(barrier, SP + 1)

    def across(v):
        return lax.rem(v + 4 + (1 - 2 * lax.rem(v, 2)) * (1 - 2 * c), 4)
    q_copies = []
    for mask in range(7, 0, -1):
        zd = across(z) if mask & 4 else z
        yd = across(y_at) if mask & 2 else y_at
        xd = across(x_at) if mask & 1 else x_at
        mine = q_all.at[pl.ds(q_rows(label), 3 * N_ROWS)]
        q_copies.append(pltpu.make_async_remote_copy(
            src_ref=mine, dst_ref=mine, send_sem=q_send.at[mask - 1], recv_sem=q_recv.at[mask - 1],
            device_id={'sp': zd * PLANE + yd * 4 + xd}, device_id_type=MESH))
    for cp in q_copies:
        cp.start()

    for cp in wkv_copies:
        cp.wait()
    kv = jnp.dot(normed[...], wkvbuf[...], preferred_element_type=F32)
    k_new = rotate((kv[:, :D] + bk_ref[...].astype(F32)).astype(BF16).astype(F32))
    v_new = (kv[:, D:] + bv_ref[...].astype(F32)).astype(BF16)
    kn_rows[...] = k_new.astype(F32)
    vn_rows[...] = v_new.astype(F32)
    for step in range(4):
        for cp in kv_copies(step):
            cp.wait()
    for cp in wo_copies:
        cp.start()
    for cp in q_copies:
        cp.wait_recv()

    lane = lax.broadcasted_iota(jnp.int32, (SLOT, D), 1)
    sub = lax.broadcasted_iota(jnp.int32, (SLOT, D), 0)
    eye = lane == sub
    pos = s * S_DEV + lax.broadcasted_iota(jnp.int32, (2 * SLOT, S_DEV), 1)

    def rs_copy(dest):
        return pltpu.make_async_remote_copy(
            src_ref=o_send.at[dest], dst_ref=o_recv.at[pl.ds(pl.multiple_of(s * SLOT, SLOT), SLOT)],
            send_sem=rs_send, recv_sem=rs_recv, device_id={'sp': dest}, device_id_type=MESH)

    def rows_step(step, carry):
        y_to = lax.rem(y_at + far_rows(step), 4)
        work = []
        for u in range(4):
            for r in range(2):
                chip = 4 * y_to + lax.rem(x_at + (2, 1, 3, 0)[u], 4)
                work.append((u, r, chip, chip + PLANE * r))
        scores = []
        for u, r, chip, b in work:
            sc = lax.dot_general(q_all[pl.ds(b, 2 * SLOT, stride=N_ROWS), :].astype(BF16), kbuf[b],
                                 (((1,), (1,)), ((), ())), preferred_element_type=F32)
            scores.append(jnp.where(pos < seq_ref[b], sc, NEG_BIG))
        tops = [jnp.max(sc, axis=1, keepdims=True) for sc in scores]
        probs = [jnp.exp2((sc - m) * qk_scale) for sc, m in zip(scores, tops)]
        sums = [jnp.sum(pr, axis=1, keepdims=True) for pr in probs]
        parts = list(zip(work, tops, sums, probs))
        for group in (parts[:4], parts[4:]):
            for (u, r, chip, b), m, l, pr in group:
                o = jnp.dot(pr.astype(BF16), vbuf[b], preferred_element_type=F32)
                m2 = m * qk_scale
                for hf in range(2):
                    part = slice(hf * SLOT, (hf + 1) * SLOT)
                    m_row = jnp.sum(jnp.where(eye, m2[part], 0.0), axis=0, keepdims=True)
                    l_row = jnp.sum(jnp.where(eye, l[part], 0.0), axis=0, keepdims=True)
                    o_send[(2 * r + hf) * PLANE + chip] = jnp.where(
                        sub == HALF, m_row, jnp.where(sub == HALF + 1, l_row, o[part]))
            for (u, r, chip, b), m, l, pr in group:
                for hf in range(2):
                    dest = (2 * r + hf) * PLANE + chip
                    if u < 3:
                        rs_copy(dest).start()
                    else:
                        @pl.when(dest != s)
                        def _():
                            rs_copy(dest).start()
        return carry
    lax.fori_loop(0, 4, rows_step, 0)
    mine = pl.ds(pl.multiple_of(s * SLOT, SLOT), SLOT)
    o_recv[mine, :] = o_send[s]

    my_row = p + PLANE * lax.div(z, 2)
    q_own = q_all[pl.ds(my_half * SLOT * N_ROWS + my_row, SLOT, stride=N_ROWS), :]
    k_mine = kn_rows[pl.ds(my_row, 1), :]
    v_mine = vn_rows[pl.ds(my_row, 1), :]
    s_new = jnp.sum(q_own * k_mine, axis=1, keepdims=True) * qk_scale

    def all_in(ref, sem):
        pltpu.make_async_copy(ref, ref, sem).wait()

    all_in(o_recv.at[pl.ds(0, (SP - 1) * SLOT)], rs_recv)
    m_rows = o_recv[pl.ds(HALF, SP, stride=SLOT), :]
    l_rows = o_recv[pl.ds(HALF + 1, SP, stride=SLOT), :]
    stats = jnp.transpose(jnp.concatenate([m_rows, l_rows], axis=0))[:SLOT]
    m_cols, l_cols = stats[:, :SP], stats[:, SP:]
    m_top = jnp.maximum(jnp.max(m_cols, axis=1, keepdims=True), s_new)
    w_cols = jnp.exp2(m_cols - m_top)
    w_new = jnp.exp2(s_new - m_top)
    l_all = jnp.sum(w_cols * l_cols, axis=1, keepdims=True) + w_new
    acc = w_new * v_mine
    for j in range(SP):
        acc = acc + w_cols[:, j:j + 1] * o_recv[j * SLOT:(j + 1) * SLOT, :]
    attn = acc / l_all
    lhs[...] = jnp.zeros_like(lhs)
    for j in range(HALF):
        lhs[0:1, j * D:(j + 1) * D] = attn[j:j + 1, :]
    for cp in wo_copies:
        cp.wait()

    lhs_b16 = lhs[...].astype(BF16)

    def product(half, place):
        for n in range(N_OUT // 2 // N_CUT):
            cols = pl.ds(pl.multiple_of(half * (N_OUT // 2) + n * N_CUT, N_CUT), N_CUT)
            piece = jnp.dot(lhs_b16, wobuf[:, cols], preferred_element_type=F32)
            for j in range(N_CUT // D):
                part[place, n * (N_CUT // D) + j:n * (N_CUT // D) + j + 1, :] = piece[0:1, j * D:(j + 1) * D]

    def x_copy(n, place, target):
        return pltpu.make_async_remote_copy(
            src_ref=part.at[place], dst_ref=others.at[n], send_sem=x_send.at[n], recv_sem=x_recv.at[n],
            device_id=target, device_id_type=MESH)
    x_copies = [x_copy(0, 1, {'sp': near, 'tp': 1 - c}), x_copy(1, 1, {'sp': near}), x_copy(2, 0, {'tp': 1 - c})]
    product(1 - my_half, 1)
    x_copies[0].start()
    x_copies[1].start()
    product(my_half, 0)
    x_copies[2].start()
    for cp in x_copies:
        cp.wait_recv()

    def ag_slot(i):
        return ag.at[pl.ds(pl.multiple_of(i * AG, 8), AG)]
    ag[pl.ds(pl.multiple_of(s * AG, 8), AG), :] = (part[0] + others[2]) + (others[0] + others[1])

    offsets = sorted(((dz, dy, j) for dz in range(4) for dy in range(4) for j in range(2)),
                     key=lambda d: min(d[0], 4 - d[0]) + min(d[1], 4 - d[1]) + 1.5 * d[2])

    def ag_copy(n):
        dz, dy, j = offsets[n]
        return pltpu.make_async_remote_copy(
            src_ref=ag_slot(s), dst_ref=ag_slot(s), send_sem=ag_send, recv_sem=ag_recv.at[n],
            device_id={'sp': chip_at(dz, dy, 2 * j + c)}, device_id_type=MESH)

    def forward(n):
        dz, dy, j = offsets[n]
        slot = ag_slot(chip_at(4 - dz, 4 - dy, 4 - 2 * j - c))
        return slot, pltpu.make_async_remote_copy(
            src_ref=slot, dst_ref=slot, send_sem=f_send, recv_sem=f_recv, device_id={'tp': 1 - c}, device_id_type=MESH)

    def relay(n):
        slot, cp = forward(n)
        pltpu.make_async_copy(slot, slot, ag_recv.at[n]).wait()
        cp.start()

    def to_first_row(n):
        dz, dy, j = offsets[n]
        return jnp.logical_and(lax.rem(z + dz, 4) == 0, lax.rem(y_at + dy, 4) == 0)

    def ag_starts(wanted):
        for n in range(SP // 2 - 1, -1, -1):
            go = wanted(n) if n else jnp.logical_and(wanted(n), c == 1)

            @pl.when(go)
            def _():
                ag_copy(n).start()
    ag_starts(to_first_row)
    ag_starts(lambda n: jnp.logical_not(to_first_row(n)))

    @pl.when(c == 1)
    def _():
        relay(0)
    for n in range(1, SP // 2):
        relay(n)

    few, many = ag.at[pl.ds(0, (SP // 2 - 1) * AG)], ag.at[pl.ds(0, SP // 2 * AG)]

    @pl.when(c == 0)
    def _():
        all_in(many, f_recv)
        all_in(few, f_send)
        all_in(few, ag_send)

    @pl.when(c == 1)
    def _():
        all_in(few, f_recv)
        all_in(many, f_send)
        all_in(many, ag_send)
    all_in(o_send.at[pl.ds(0, SP - 1)], rs_send)
    for cp in q_copies + x_copies:
        cp.wait_send()


def step_call(freq, *operands):
    hidden, norm_w, w_q, b_q, w_k, b_k, w_v, b_v, w_o, k_cache, v_cache, positions, seq_lens = operands
    vmem = pl.BlockSpec(memory_space=pltpu.VMEM)
    hbm = pl.BlockSpec(memory_space=pltpu.HBM)
    dma = pltpu.SemaphoreType.DMA
    return pl.pallas_call(
        step_kernel,
        out_shape=(jax.ShapeDtypeStruct((SP * AG, D), F32),
                   jax.ShapeDtypeStruct((N_ROWS, D), F32), jax.ShapeDtypeStruct((N_ROWS, D), F32)),
        in_specs=[hbm, hbm, hbm, hbm, hbm, vmem, hbm, hbm, hbm, hbm, hbm, hbm, hbm, hbm],
        out_specs=(vmem, vmem, vmem),
        scratch_shapes=[
            pltpu.VMEM((N_OUT // D, D), BF16),
            pltpu.VMEM((24, D), BF16),
            pltpu.VMEM((1, D), BF16),
            pltpu.VMEM((1, D), BF16),
            pltpu.VMEM((1, N_ROWS), jnp.int32),
            pltpu.SMEM((N_ROWS,), jnp.int32),
            pltpu.VMEM((N_ROWS, N_OUT), BF16),
            pltpu.VMEM((N_ROWS, N_OUT), BF16),
            pltpu.VMEM((N_OUT, Q_DEV), BF16),
            pltpu.VMEM((N_OUT, 2 * D), BF16),
            pltpu.VMEM((24, D), F32),
            pltpu.VMEM((2 * SLOT * N_ROWS, D), F32),
            pltpu.VMEM((N_ROWS, S_DEV, D), BF16),
            pltpu.VMEM((N_ROWS, S_DEV, D), BF16),
            pltpu.VMEM((K_HALF, N_OUT), BF16),
            pltpu.VMEM((2 * N_ROWS, SLOT, D), F32),
            pltpu.VMEM((SP * SLOT, D), F32),
            pltpu.VMEM((8, K_HALF), F32),
            pltpu.VMEM((2, AG, D), F32),
            pltpu.VMEM((3, AG, D), F32),
            dma((6,)), dma, dma((N_OUT // K_CUT,)), dma((2,)), dma((7,)), dma((7,)),
            dma((8,)), dma((8,)), dma((8,)), dma, dma, dma((3,)), dma((3,)),
            dma, dma((SP // 2,)), dma, dma,
        ],
        compiler_params=pltpu.CompilerParams(
            collective_id=0, has_side_effects=True, vmem_limit_bytes=44 * 1024 * 1024),
        name='decode_step',
    )(*(x if x is freq else pltpu.with_memory_space_constraint(x, pltpu.HBM) for x in (
        hidden, norm_w.reshape(-1, D), b_q.reshape(-1, D), b_k.reshape(1, -1), b_v.reshape(1, -1), freq,
        positions.reshape(1, -1), seq_lens, w_q, w_k, w_v,
        k_cache.reshape(N_ROWS, S_DEV, D), v_cache.reshape(N_ROWS, S_DEV, D), w_o)))


def finish_kernel(ag, kn_rows, vn_rows, hid_ref, y_hbm, kn_hbm, vn_hbm, y_ref, kn_ref, vn_ref, sems):
    kn_ref[...] = kn_rows[...].astype(BF16)
    vn_ref[...] = vn_rows[...].astype(BF16)
    copies = [pltpu.make_async_copy(kn_ref, kn_hbm, sems.at[0]), pltpu.make_async_copy(vn_ref, vn_hbm, sems.at[1])]
    for zz in range(4):
        r, hf = zz // 2, zz % 2
        rows = slice(PLANE * r, PLANE * (r + 1))
        for blk in range(AG):
            col = slice(hf * (N_OUT // 2) + blk * D, hf * (N_OUT // 2) + (blk + 1) * D)
            y_blk = ag[pl.ds(zz * PLANE * AG + blk, PLANE, stride=AG), :]
            y_ref[rows, col] = (hid_ref[rows, col].astype(F32) + y_blk).astype(BF16)
        block = (pl.ds(PLANE * r, PLANE), pl.ds(hf * (N_OUT // 2), N_OUT // 2))
        copies.append(pltpu.make_async_copy(y_ref.at[block], y_hbm.at[block], sems.at[2 + zz]))
        if zz == 0:
            copies[0].start()
            copies[1].start()
        copies[-1].start()
    for cp in copies:
        cp.wait()


def finish(ag, kn_rows, vn_rows, hidden):
    vmem = pl.BlockSpec(memory_space=pltpu.VMEM)
    hbm = pl.BlockSpec(memory_space=pltpu.HBM)
    return pl.pallas_call(
        finish_kernel,
        out_shape=(jax.ShapeDtypeStruct((N_ROWS, N_OUT), BF16),
                   jax.ShapeDtypeStruct((N_ROWS, D), BF16), jax.ShapeDtypeStruct((N_ROWS, D), BF16)),
        in_specs=[vmem] * 4, out_specs=(hbm,) * 3,
        scratch_shapes=[pltpu.VMEM((N_ROWS, N_OUT), BF16), pltpu.VMEM((N_ROWS, D), BF16),
                        pltpu.VMEM((N_ROWS, D), BF16), pltpu.SemaphoreType.DMA((6,))],
        compiler_params=pltpu.CompilerParams(vmem_limit_bytes=8 * 1024 * 1024),
        name='finish',
    )(ag, kn_rows, vn_rows, hidden)


def solution(mesh):
    def device_step(*operands):
        lane = jnp.arange(D, dtype=jnp.int32)
        inv_freq = ROPE_BASE ** (-2.0 * (lane // 2).astype(jnp.float32) / (D // 2))
        freq = jnp.where(lane < D // 2, inv_freq, 0.0).reshape(1, D)
        y_out, k_new, v_new = finish(*step_call(freq, *operands), operands[0])
        return y_out, k_new.reshape(N_ROWS, 1, D), v_new.reshape(N_ROWS, 1, D)

    col_spec = P(None, 'tp')
    vec_spec = P('tp')
    cache_spec = P('dp', 'sp', 'tp', None)
    group_spec = P('dp', 'tp', None)
    in_specs = (P('dp', None), P(None), col_spec, vec_spec, col_spec, vec_spec, col_spec, vec_spec,
                P('tp', None), cache_spec, cache_spec, P('dp'), P('dp'))
    out_specs = (P('dp', None), group_spec, group_spec)
    return jax.shard_map(device_step, mesh=mesh, in_specs=in_specs, out_specs=out_specs, check_vma=False)
```
